16 devices in a mesh: stage: 2 (over z), expert: 8 (over y, x, core).
Axes of the slice: x: 2, y: 2, z: 2, core: 2. Of those that a mesh axis runs over, the one named last changes fastest.
Arguments:
- x_acts: bfloat16 [2, 8192, 1024], P('stage', 'expert')
- expert_ids: int32 [2, 8192, 2], P('stage', 'expert')
- gate_vals: float32 [2, 8192, 2], P('stage', 'expert')
- w_gate: bfloat16 [2, 8, 1024, 1536], P('stage', 'expert')
- w_up: bfloat16 [2, 8, 1024, 1536], P('stage', 'expert')
- w_down: bfloat16 [2, 8, 1536, 1024], P('stage', 'expert')
- grad_out: bfloat16 [2, 8192, 1024], P('stage', 'expert')
Outputs:
- output 1: bfloat16 [2, 8192, 1024], P('stage', 'expert')
- output 2: bfloat16 [2, 8192, 1024], P('stage', 'expert')
- output 3: bfloat16 [2, 8, 1024, 1536], P('stage', 'expert')
- output 4: bfloat16 [2, 8, 1024, 1536], P('stage', 'expert')
- output 5: bfloat16 [2, 8, 1536, 1024], P('stage', 'expert')
All inputs are finite; a program needn't handle non-finite values.
Results may differ from the reference program's by a relative error of at most 0.00856692.
Values are sent between devices in bfloat16 or wider.
A program may use at most 1 GiB of HBM per device.

```python
import jax
import jax.numpy as jnp
from jax import lax

STAGES = 2
EXPERT_DEVS = 8
TOK_DEV = 1024
MODEL_DIM = 1024
FFN_DIM = 1536
EXPERTS = 8
TOP_K = 2
GROUPS = 1
TOP_GROUPS = 1
NOISE_SPAN = 256

TOKENS = EXPERT_DEVS * TOK_DEV
CAPACITY = 2 * TOK_DEV * TOP_K // EXPERTS + 1
GROUP_SIZE = EXPERTS // GROUPS


def draw_routing(key):
    hot_key, tok_key = jax.random.split(key)
    hot_mask = jax.random.permutation(hot_key, EXPERTS) < GROUPS
    hot_bonus = jnp.where(hot_mask, (CAPACITY + 1) * NOISE_SPAN, 0)
    group_big = (2 * CAPACITY + 3) * NOISE_SPAN
    expert_range = jnp.arange(EXPERTS)
    group_range = jnp.arange(GROUPS)

    def one_device(dev_key):
        def draw_step(load_now, tok_pos):
            tok_noise = jax.random.randint(jax.random.fold_in(dev_key, tok_pos), (EXPERTS,), 0, NOISE_SPAN)
            room_left = CAPACITY - load_now
            raw_score = jnp.where(room_left > 0, hot_bonus + room_left * NOISE_SPAN + tok_noise, -1)
            per_group = raw_score.reshape(GROUPS, GROUP_SIZE)
            open_count = jnp.sum(per_group >= 0, axis=1)
            group_score = (jnp.minimum(open_count, TOP_K) * group_big + jnp.max(per_group, axis=1)) * GROUPS + group_range
            picked_groups = lax.top_k(group_score, TOP_GROUPS)[1]
            group_open = jnp.any(group_range[:, None] == picked_groups[None, :], axis=1)
            allowed = jnp.repeat(group_open, GROUP_SIZE)
            final_score = jnp.where(allowed, raw_score, -1) * EXPERTS + expert_range
            chosen = lax.top_k(final_score, TOP_K)[1]
            new_load = load_now + jnp.sum(chosen[:, None] == expert_range[None, :], axis=0).astype(jnp.int32)
            return new_load, chosen.astype(jnp.int32)

        return lax.scan(draw_step, jnp.zeros((EXPERTS,), jnp.int32), jnp.arange(TOK_DEV))[1]

    dev_keys = jax.random.split(tok_key, STAGES * EXPERT_DEVS)
    return jax.vmap(one_device)(dev_keys).reshape(STAGES, TOKENS, TOP_K)


def setup_inputs(seed: int = 0) -> dict:
    draw_keys = jax.random.split(jax.random.key(seed), 7)
    tok_shape = (STAGES, TOKENS, MODEL_DIM)
    up_shape = (STAGES, EXPERTS, MODEL_DIM, FFN_DIM)
    x_acts = jax.random.normal(draw_keys[0], tok_shape, jnp.float32).astype(jnp.bfloat16)
    expert_ids = draw_routing(draw_keys[1])
    gate_vals = jax.random.uniform(draw_keys[2], (STAGES, TOKENS, TOP_K), jnp.float32, minval=0.5, maxval=1.5) * TOP_K ** -0.5
    w_gate = (jax.random.normal(draw_keys[3], up_shape, jnp.float32) * MODEL_DIM ** -0.5).astype(jnp.bfloat16)
    w_up = (jax.random.normal(draw_keys[4], up_shape, jnp.float32) * MODEL_DIM ** -0.5).astype(jnp.bfloat16)
    w_down = (jax.random.normal(draw_keys[5], (STAGES, EXPERTS, FFN_DIM, MODEL_DIM), jnp.float32) * FFN_DIM ** -0.5).astype(jnp.bfloat16)
    grad_out = jax.random.normal(draw_keys[6], tok_shape, jnp.float32).astype(jnp.bfloat16)
    return {'x_acts': x_acts, 'expert_ids': expert_ids, 'gate_vals': gate_vals, 'w_gate': w_gate, 'w_up': w_up, 'w_down': w_down, 'grad_out': grad_out}


def expert_pass(expert_in):
    x_rows, do_rows, wg_mat, wu_mat, wd_mat = expert_in
    pre_gate = jnp.dot(x_rows, wg_mat, preferred_element_type=jnp.float32)
    pre_up = jnp.dot(x_rows, wu_mat, preferred_element_type=jnp.float32)
    sig_gate = jax.nn.sigmoid(pre_gate)
    act_gate = pre_gate * sig_gate
    hidden = (act_gate * pre_up).astype(jnp.bfloat16)
    out_rows = jnp.dot(hidden, wd_mat, preferred_element_type=jnp.float32).astype(jnp.bfloat16)
    g_hidden = jnp.dot(do_rows, wd_mat.T, preferred_element_type=jnp.float32)
    g_up = (g_hidden * act_gate).astype(jnp.bfloat16)
    g_pre = (g_hidden * pre_up * sig_gate * (1.0 + pre_gate * (1.0 - sig_gate))).astype(jnp.bfloat16)
    dx_rows = (jnp.dot(g_pre, wg_mat.T, preferred_element_type=jnp.float32) + jnp.dot(g_up, wu_mat.T, preferred_element_type=jnp.float32)).astype(jnp.bfloat16)
    g_wgate = jnp.dot(x_rows.T, g_pre, preferred_element_type=jnp.float32).astype(jnp.bfloat16)
    g_wup = jnp.dot(x_rows.T, g_up, preferred_element_type=jnp.float32).astype(jnp.bfloat16)
    g_wdown = jnp.dot(hidden.T, do_rows, preferred_element_type=jnp.float32).astype(jnp.bfloat16)
    return out_rows, dx_rows, g_wgate, g_wup, g_wdown


def stage_pass(stage_in):
    x_in, ids_in, gates_in, wg_all, wu_all, wd_all, dy_stage = stage_in
    ids_src = ids_in.reshape(EXPERT_DEVS, TOK_DEV * TOP_K)
    expert_range = jnp.arange(EXPERTS)

    def src_positions(ids_row):
        one_hot = (ids_row[:, None] == expert_range[None, :]).astype(jnp.int32)
        ranks = jnp.cumsum(one_hot, axis=0) - 1
        return jnp.sum(ranks * one_hot, axis=1)

    positions = lax.map(src_positions, ids_src)
    src_index = jnp.arange(EXPERT_DEVS)[:, None]
    slots = ((ids_src * EXPERT_DEVS + src_index) * CAPACITY + positions).reshape(TOKENS, TOP_K)
    flat_slots = slots.reshape(-1)
    row_count = EXPERTS * EXPERT_DEVS * CAPACITY
    tok_of_choice = jnp.repeat(jnp.arange(TOKENS, dtype=jnp.int32), TOP_K)
    row_token = jnp.zeros((row_count,), jnp.int32).at[flat_slots].set(tok_of_choice + 1) - 1
    row_gate = jnp.zeros((row_count,), jnp.float32).at[flat_slots].set(gates_in.reshape(-1))
    safe_token = jnp.maximum(row_token, 0)
    x_rows = jnp.where((row_token >= 0)[:, None], x_in[safe_token], jnp.zeros((), jnp.bfloat16))
    do_rows = (row_gate[:, None] * dy_stage[safe_token].astype(jnp.float32)).astype(jnp.bfloat16)
    rows_shape = (EXPERTS, EXPERT_DEVS * CAPACITY, MODEL_DIM)
    out_rows, dx_rows, g_wgate, g_wup, g_wdown = lax.map(expert_pass, (x_rows.reshape(rows_shape), do_rows.reshape(rows_shape), wg_all, wu_all, wd_all))
    out_flat = out_rows.reshape(row_count, MODEL_DIM).astype(jnp.float32)
    dx_flat = dx_rows.reshape(row_count, MODEL_DIM).astype(jnp.float32)
    moe_out = jnp.sum(gates_in[:, :, None] * out_flat[slots], axis=1).astype(jnp.bfloat16)
    grad_in = jnp.sum(dx_flat[slots], axis=1).astype(jnp.bfloat16)
    return moe_out, grad_in, g_wgate, g_wup, g_wdown


def reference(x_acts, expert_ids, gate_vals, w_gate, w_up, w_down, grad_out):
    stage_in = (jnp.roll(x_acts, 1, axis=0), jnp.roll(expert_ids, 1, axis=0), jnp.roll(gate_vals, 1, axis=0), w_gate, w_up, w_down, grad_out)
    moe_out, grad_in, grad_w_gate, grad_w_up, grad_w_down = lax.map(stage_pass, stage_in)
    return moe_out, jnp.roll(grad_in, -1, axis=0), grad_w_gate, grad_w_up, grad_w_down
```

```python
import functools

import jax
import jax.numpy as jnp
from jax import lax
from jax.experimental import pallas as pl
from jax.experimental.pallas import tpu as pltpu
from jax.sharding import PartitionSpec as P

MESH = pl.DeviceIdType.MESH
BF16 = jnp.bfloat16
F32 = jnp.float32
NN = (((1,), (0,)), ((), ()))
NT = (((1,), (1,)), ((), ()))
TN = (((0,), (0,)), ((), ()))
DEVS = 8
TILE = 512


def mm(lhs, rhs, dims=NN):
    return lax.dot_general(lhs, rhs, dims, preferred_element_type=F32)


def flip(a, b):
    out = 0
    for w in (1, 2, 4):
        p = (a // w) % 2
        q = (b // w) % 2
        out = out + w * (p + q - 2 * p * q)
    return out


def nth_offset(k):
    third, fourth = k // 3, k // 4
    return k + (third - fourth) * (1 - k // 6) - (fourth - k // 5)


def col(start, size):
    return pl.ds(pl.multiple_of(start, size), size)


def moe_kernel(rows, sent, tab_ref, x_ref, dy_ref, wg_hbm, wu_hbm, wd_hbm,
               y_ref, dx_ref, gwg_ref, gwu_ref, gwd_ref, xg, dyg, out_stage, dx_stage, out_back, dx_back,
               tabs, pos_s, gate_s, pos_y, gate_y, pos_x, wg, wu, wd, accg, accu, accd, xst, dyst, onehot, grow,
               xr, dor, hid, da, du, obuf, dbuf,
               load_sem, tab_send, tab_recv, z_send, x_send, dy_send, x_recv, dy_recv,
               out_send, out_recv, dxs_send, dxs_recv, loc_sem):
    tok, dim = x_ref.shape
    ffn = wg_hbm.shape[1]
    half = tok // 2
    st, me = lax.axis_index('stage'), lax.axis_index('expert')
    other = 1 - st
    part = [pl.ds(0, half), pl.ds(half, half)]

    barrier = pltpu.get_barrier_semaphore()
    for d in range(DEVS):
        if d:
            pl.semaphore_signal(barrier, inc=1, device_id=(st, flip(me, d)), device_id_type=MESH)
        pl.semaphore_signal(barrier, inc=1, device_id=(other, flip(me, d)), device_id_type=MESH)
    pl.semaphore_wait(barrier, 2 * DEVS - 1)

    def remote(src, dst, ssem, rsem, stage, dev):
        return pltpu.make_async_remote_copy(src_ref=src, dst_ref=dst, send_sem=ssem, recv_sem=rsem,
                                            device_id=(stage, dev), device_id_type=MESH)

    def push(src, dst, ssem, rsem, stage, dev):
        remote(src, dst, ssem, rsem, stage, dev).start()

    def tab_copy(d):
        return remote(tab_ref, tabs.at[d], tab_send.at[d], tab_recv.at[d], other, flip(me, d))

    for d in range(DEVS):
        tab_copy(d).start()
    loads = [pltpu.make_async_copy(src, dst, load_sem.at[n])
             for n, (src, dst) in enumerate(((wg_hbm, wg), (wu_hbm, wu), (wd_hbm, wd)))]
    for c in range(2):
        push(x_ref.at[part[c]], xg.at[0, part[c]], z_send.at[c], x_recv.at[0, c], other, me)
    for c in range(2):
        for n, b in enumerate((2, 4, 1)):
            push(dy_ref.at[part[c]], dyg.at[b, part[c]], dy_send.at[2 * n + c], dy_recv.at[b, c], st, flip(me, b))
    for cp in loads:
        cp.start()

    def got(buf, sems, d, c):
        remote(buf.at[d, part[c]], buf.at[d, part[c]], z_send.at[0], sems.at[d, c], st, me).wait_recv()

    @pl.loop(0, tok // 128)
    def _(n):
        accg[col(n * 128, 128), :] = jnp.zeros((128, ffn), F32)
        accu[col(n * 128, 128), :] = jnp.zeros((128, ffn), F32)

    @pl.loop(0, ffn // 128)
    def _(n):
        accd[col(n * 128, 128), :] = jnp.zeros((128, dim), F32)

    xst[...] = jnp.where(lax.broadcasted_iota(jnp.int32, (tok, tok), 0) < lax.broadcasted_iota(jnp.int32, (tok, tok), 1),
                         1.0, 0.0).astype(BF16)
    for d in range(DEVS):
        tab_copy(d).wait_recv()

    def plan(id0, id1, g0, g1, wanted):
        first, second = id0 == wanted, id1 == wanted
        named = jnp.logical_or(first, second)
        before = mm(jnp.where(named, 1.0, 0.0).astype(BF16), xst[...])
        return jnp.where(named, before, -1.0), jnp.where(first, g0, jnp.where(second, g1, 0.0))

    sub = lax.broadcasted_iota(jnp.int32, (DEVS, tok), 0)
    mine = jnp.zeros((DEVS, tok), F32) + me.astype(F32)
    each = jnp.bitwise_xor(sub, me).astype(F32)
    seen = tabs[...]
    pos, gate = plan(seen[:, 0, :], seen[:, 1, :], seen[:, 2, :], seen[:, 3, :], mine)
    for d in range(DEVS):
        pos_s[d] = pos[d:d + 1].astype(jnp.int32)
        gate_s[d] = gate[d:d + 1]
    here = tabs[0]
    pos, gate = plan(here[0:1], here[1:2], here[2:3], here[3:4], each)
    pos_y[...] = pos.T
    gate_y[...] = gate.T
    own = tab_ref[...]
    pos, _ = plan(own[0:1], own[1:2], own[2:3], own[3:4], each)
    pos_x[...] = pos.T

    for c in range(2):
        got(xg, x_recv, 0, c)
        for n, b in enumerate((2, 4, 1)):
            push(xg.at[0, part[c]], xg.at[b, part[c]], x_send.at[2 * n + c], x_recv.at[b, c], st, flip(me, b))

    def pass_on(buf, ssem, rsem):
        for d, to, c_on, n in ((2, 4, 1, 6), (4, 2, 0, 7)):
            for c in range(2):
                got(buf, rsem, d, c)
            push(buf.at[d, part[c_on]], buf.at[6, part[c_on]], ssem.at[n], rsem.at[6, c_on], st, flip(me, to))
        for m, d in enumerate((2, 4)):
            for c in range(2):
                push(buf.at[d, part[c]], buf.at[d + 1, part[c]], ssem.at[8 + 2 * m + c], rsem.at[d + 1, c], st, flip(me, 1))

    def pass_last(buf, ssem, rsem):
        for c in range(2):
            got(buf, rsem, 6, c)
            push(buf.at[6, part[c]], buf.at[7, part[c]], ssem.at[12 + c], rsem.at[7, c], st, flip(me, 1))

    pass_on(dyg, dy_send, dy_recv)
    for cp in loads:
        cp.wait()

    def out_copy(d):
        return remote(out_stage.at[d], out_back.at[d], out_send.at[d], out_recv.at[d], st, flip(me, d))

    def dx_copy(d):
        return remote(dx_stage.at[d], dx_back.at[d], dxs_send.at[d], dxs_recv.at[d], other, flip(me, d))

    def local(src, dst, n):
        return pltpu.make_async_copy(src, dst, loc_sem.at[n])

    third = rows // 3

    @pl.loop(0, DEVS)
    def _(k):
        d = nth_offset(k)

        @pl.when(k == 2)
        def _():
            pass_on(xg, x_send, x_recv)

        @pl.when(k == 4)
        def _():
            pass_last(dyg, dy_send, dy_recv)

        @pl.when(k == 5)
        def _():
            pass_last(xg, x_send, x_recv)

        @pl.when(d % 2 == 1)
        def _():
            for c in range(2):
                got(xg, x_recv, d, c)
                got(dyg, dy_recv, d, c)

        local(xg.at[d], xst, 0).start()

        @pl.when(k == 0)
        def _():
            local(dy_ref, dyst, 1).start()

        @pl.when(k > 0)
        def _():
            local(dyg.at[d], dyst, 1).start()

        @pl.loop(0, 3)
        def _(n):
            place = lax.broadcasted_iota(jnp.int32, (third, tok), 0) + n * third
            hit = place == pos_s[d]
            span = col(n * third, third)
            onehot[span, :] = jnp.where(hit, 1.0, 0.0).astype(BF16)
            grow[span, :] = jnp.sum(jnp.where(hit, gate_s[d], 0.0), axis=1, keepdims=True)

        local(xg.at[d], xst, 0).wait()
        local(dyg.at[d], dyst, 1).wait()

        @pl.loop(0, dim // TILE)
        def _(n):
            span = col(n * TILE, TILE)
            xr[:, span] = mm(onehot[...], xst[:, span]).astype(BF16)
            dor[:, span] = (grow[...] * mm(onehot[...], dyst[:, span])).astype(BF16)

        @pl.loop(0, ffn // TILE)
        def _(n):
            span = col(n * TILE, TILE)
            a = mm(xr[...], wg[:, span])
            u = mm(xr[...], wu[:, span])
            gh = mm(dor[...], wd[span, :], NT)
            sig = jax.nn.sigmoid(a)
            act = a * sig
            hid[:, span] = (act * u).astype(BF16)
            du[:, span] = (gh * act).astype(BF16)
            da[:, span] = (gh * u * sig * (1.0 + a * (1.0 - sig))).astype(BF16)

        @pl.loop(0, dim // TILE)
        def _(n):
            span = col(n * TILE, TILE)
            obuf[:, span] = mm(hid[...], wd[:, span]).astype(BF16)

        @pl.when(k == 0)
        def _():
            local(obuf, out_back.at[0], 0).start()

        @pl.when(k > 0)
        def _():
            local(obuf, out_stage.at[d], 0).start()

        @pl.loop(0, dim // TILE)
        def _(n):
            span = col(n * TILE, TILE)
            dbuf[:, span] = (mm(da[...], wg[span, :], NT) + mm(du[...], wu[span, :], NT)).astype(BF16)

        local(dbuf, dx_stage.at[d], 1).start()
        local(obuf, out_stage.at[d], 0).wait()

        @pl.when(k > 0)
        def _():
            out_copy(d).start()

        local(dbuf, dx_stage.at[d], 1).wait()
        dx_copy(d).start()

        @pl.loop(0, dim // TILE)
        def _(m):
            over = col(m * TILE, TILE)

            @pl.loop(0, ffn // TILE)
            def _(n):
                span = col(n * TILE, TILE)
                accg[over, span] += mm(xr[:, over], da[:, span], TN)
                accu[over, span] += mm(xr[:, over], du[:, span], TN)
                accd[span, over] += mm(hid[:, span], dor[:, over], TN)

    for acc, buf in ((accg, wg), (accu, wu), (accd, wd)):
        @pl.loop(0, acc.shape[0] // 128)
        def _(n, acc=acc, buf=buf):
            span = col(n * 128, 128)
            buf[span, :] = acc[span, :].astype(BF16)
    stores = [pltpu.make_async_copy(src, dst, load_sem.at[n])
              for n, (src, dst) in enumerate(((wg, gwg_ref), (wu, gwu_ref), (wd, gwd_ref)))]
    for cp in stores:
        cp.start()

    @pl.loop(0, tok // 128)
    def _(n):
        accg[col(n * 128, 128), :] = jnp.zeros((128, ffn), F32)
        accu[col(n * 128, 128), :] = jnp.zeros((128, ffn), F32)

    @pl.loop(0, DEVS)
    def _(k):
        d = nth_offset(k)

        @pl.when(k > 0)
        def _():
            out_copy(d).wait_recv()

        dx_copy(d).wait_recv()
        local(out_back.at[d], obuf, 0).start()
        local(dx_back.at[d], dbuf, 1).start()
        local(out_back.at[d], obuf, 0).wait()
        local(dx_back.at[d], dbuf, 1).wait()

        @pl.loop(0, tok // 256)
        def _(n):
            over = col(n * 256, 256)
            place = lax.broadcasted_iota(jnp.int32, (256, rows), 1)
            lane = lax.broadcasted_iota(jnp.int32, (256, DEVS), 1) == d

            def pick(ref):
                return jnp.sum(jnp.where(lane, ref[over, :], 0.0), axis=1, keepdims=True)

            sel = jnp.where(place == pick(pos_y).astype(jnp.int32), 1.0, 0.0).astype(BF16)
            accg[over, 0:dim] += pick(gate_y) * mm(sel, obuf[...])
            sel = jnp.where(place == pick(pos_x).astype(jnp.int32), 1.0, 0.0).astype(BF16)
            accu[over, 0:dim] += mm(sel, dbuf[...])

    @pl.loop(0, tok // 128)
    def _(n):
        span = col(n * 128, 128)
        xst[span, :] = accg[span, 0:dim].astype(BF16)
        dyst[span, :] = accu[span, 0:dim].astype(BF16)

    ends = [local(xst, y_ref, 0), local(dyst, dx_ref, 1)]
    for cp in ends:
        cp.start()
    for cp in ends + stores:
        cp.wait()
    for sems, count in ((z_send, 2), (x_send, 14), (dy_send, 14)):
        for n in range(count):
            remote(xg.at[0, part[0]], xg.at[0, part[0]], sems.at[n], sems.at[n], st, me).wait_send()
    for d in range(DEVS):
        tab_copy(d).wait_send()
        dx_copy(d).wait_send()
        if d:
            out_copy(d).wait_send()


def moe_call(tab, x, dy, wg, wu, wd, cap):
    tok, dim = x.shape
    ffn = wg.shape[1]
    rows = -(-cap // 48) * 48
    sent = -(-cap // 8) * 8
    any_spec = pl.BlockSpec(memory_space=pl.ANY)
    vmem = pl.BlockSpec(memory_space=pltpu.VMEM)
    shape = jax.ShapeDtypeStruct
    out_shape = [shape((tok, dim), BF16)] * 2 + [shape(wg.shape, BF16), shape(wu.shape, BF16), shape(wd.shape, BF16)]
    out_shape += [shape((DEVS, tok, dim), BF16)] * 2 + [shape((DEVS, rows, dim), BF16)] * 4
    dma, vm = pltpu.SemaphoreType.DMA, pltpu.VMEM
    scratch = [
        vm((DEVS, 8, tok), F32), vm((DEVS, 1, tok), jnp.int32), vm((DEVS, 1, tok), F32),
        vm((tok, DEVS), F32), vm((tok, DEVS), F32), vm((tok, DEVS), F32),
        vm((dim, ffn), BF16), vm((dim, ffn), BF16), vm((ffn, dim), BF16),
        vm((dim, ffn), F32), vm((dim, ffn), F32), vm((ffn, dim), F32),
        vm((tok, dim), BF16), vm((tok, dim), BF16), vm((rows, tok), BF16), vm((rows, 1), F32),
        vm((rows, dim), BF16), vm((rows, dim), BF16), vm((rows, ffn), BF16), vm((rows, ffn), BF16), vm((rows, ffn), BF16),
        vm((rows, dim), BF16), vm((rows, dim), BF16),
        dma((3,)), dma((DEVS,)), dma((DEVS,)), dma((2,)), dma((14,)), dma((14,)), dma((DEVS, 2)), dma((DEVS, 2)),
        dma((DEVS,)), dma((DEVS,)), dma((DEVS,)), dma((DEVS,)), dma((2,)),
    ]
    return pl.pallas_call(
        functools.partial(moe_kernel, rows, sent),
        out_shape=out_shape,
        in_specs=[vmem] + [any_spec] * 5,
        out_specs=[any_spec] * len(out_shape),
        scratch_shapes=scratch,
        compiler_params=pltpu.CompilerParams(collective_id=0, has_side_effects=True, vmem_limit_bytes=67043328),
    )(tab, x, dy, wg, wu, wd)


def solution(mesh):
    stages, ep_size = mesh.shape['stage'], mesh.shape['expert']
    assert stages == 2 and ep_size == DEVS
    tok_spec = P('stage', 'expert', None)
    w_spec = P('stage', 'expert', None, None)

    def device_fn(x_acts, expert_ids, gate_vals, w_gate, w_up, w_down, grad_out):
        tok, top_k = expert_ids.shape[1:]
        cap = 2 * tok * top_k // (w_gate.shape[1] * ep_size) + 1
        tab = jnp.concatenate([expert_ids[0].T.astype(F32), gate_vals[0].T, jnp.zeros((4, tok), F32)], axis=0)
        outs = moe_call(tab, x_acts[0], grad_out[0], w_gate[0, 0], w_up[0, 0], w_down[0, 0], cap)
        y, dx, gwg, gwu, gwd = outs[:5]
        return y[None], dx[None], gwg[None, None], gwu[None, None], gwd[None, None]

    return jax.shard_map(device_fn, mesh=mesh, in_specs=(tok_spec, tok_spec, tok_spec, w_spec, w_spec, w_spec, tok_spec), out_specs=(tok_spec, tok_spec, w_spec, w_spec, w_spec), check_vma=False)
```

```python
import functools

import jax
import jax.numpy as jnp
from jax import lax
from jax.experimental import pallas as pl
from jax.experimental.pallas import tpu as pltpu
from jax.sharding import PartitionSpec as P

MESH = pl.DeviceIdType.MESH
BF16 = jnp.bfloat16
F32 = jnp.float32
NN = (((1,), (0,)), ((), ()))
NT = (((1,), (1,)), ((), ()))
TN = (((0,), (0,)), ((), ()))
DEVS = 8
TILE = 512


def mm(lhs, rhs, dims=NN):
    return lax.dot_general(lhs, rhs, dims, preferred_element_type=F32)


def flip(a, b):
    out = 0
    for w in (1, 2, 4):
        p = (a // w) % 2
        q = (b // w) % 2
        out = out + w * (p + q - 2 * p * q)
    return out


def nth_offset(k):
    third, fourth = k // 3, k // 4
    return k + (third - fourth) * (1 - k // 6) - (fourth - k // 5)


def col(start, size):
    return pl.ds(pl.multiple_of(start, size), size)


def moe_kernel(rows, sent, tab_ref, x_ref, dy_ref, wg_hbm, wu_hbm, wd_hbm,
               y_ref, dx_ref, gwg_ref, gwu_ref, gwd_ref, xg, dyg, out_stage, dx_stage, out_back, dx_back,
               tabs, pos_s, gate_s, pos_y, gate_y, pos_x, wg, wu, wd, accg, accu, accd, xst, dyst, onehot, grow,
               xr, dor, hid, da, du, obuf, dbuf,
               load_sem, tab_send, tab_recv, z_send, x_send, dy_send, x_recv, dy_recv,
               out_send, out_recv, dxs_send, dxs_recv, loc_sem):
    tok, dim = x_ref.shape
    ffn = wg_hbm.shape[1]
    half = tok // 2
    st, me = lax.axis_index('stage'), lax.axis_index('expert')
    other = 1 - st
    part = [pl.ds(0, half), pl.ds(half, half)]

    barrier = pltpu.get_barrier_semaphore()
    for d in range(DEVS):
        if d:
            pl.semaphore_signal(barrier, inc=1, device_id=(st, flip(me, d)), device_id_type=MESH)
        pl.semaphore_signal(barrier, inc=1, device_id=(other, flip(me, d)), device_id_type=MESH)
    pl.semaphore_wait(barrier, 2 * DEVS - 1)

    def remote(src, dst, ssem, rsem, stage, dev):
        return pltpu.make_async_remote_copy(src_ref=src, dst_ref=dst, send_sem=ssem, recv_sem=rsem,
                                            device_id=(stage, dev), device_id_type=MESH)

    def push(src, dst, ssem, rsem, stage, dev):
        remote(src, dst, ssem, rsem, stage, dev).start()

    def tab_copy(d):
        return remote(tab_ref, tabs.at[d], tab_send.at[d], tab_recv.at[d], other, flip(me, d))

    for d in range(DEVS):
        tab_copy(d).start()
    loads = [pltpu.make_async_copy(src, dst, load_sem.at[n])
             for n, (src, dst) in enumerate(((wg_hbm, wg), (wu_hbm, wu), (wd_hbm, wd)))]
    for c in range(2):
        push(x_ref.at[part[c]], xg.at[0, part[c]], z_send.at[c], x_recv.at[0, c], other, me)
    for c in range(2):
        for n, b in enumerate((2, 4, 1)):
            push(dy_ref.at[part[c]], dyg.at[b, part[c]], dy_send.at[2 * n + c], dy_recv.at[b, c], st, flip(me, b))
    for cp in loads:
        cp.start()

    def got(buf, sems, d, c):
        remote(buf.at[d, part[c]], buf.at[d, part[c]], z_send.at[0], sems.at[d, c], st, me).wait_recv()

    @pl.loop(0, tok // 128)
    def _(n):
        accg[col(n * 128, 128), :] = jnp.zeros((128, ffn), F32)
        accu[col(n * 128, 128), :] = jnp.zeros((128, ffn), F32)

    @pl.loop(0, ffn // 128)
    def _(n):
        accd[col(n * 128, 128), :] = jnp.zeros((128, dim), F32)

    xst[...] = jnp.where(lax.broadcasted_iota(jnp.int32, (tok, tok), 0) < lax.broadcasted_iota(jnp.int32, (tok, tok), 1),
                         1.0, 0.0).astype(BF16)
    for d in range(DEVS):
        tab_copy(d).wait_recv()

    def plan(id0, id1, g0, g1, wanted):
        first, second = id0 == wanted, id1 == wanted
        named = jnp.logical_or(first, second)
        before = mm(jnp.where(named, 1.0, 0.0).astype(BF16), xst[...])
        return jnp.where(named, before, -1.0), jnp.where(first, g0, jnp.where(second, g1, 0.0))

    sub = lax.broadcasted_iota(jnp.int32, (DEVS, tok), 0)
    always = jnp.zeros((DEVS, tok), F32) + me.astype(F32)
    each = jnp.bitwise_xor(sub, me).astype(F32)
    seen = tabs[...]
    pos, gate = plan(seen[:, 0, :], seen[:, 1, :], seen[:, 2, :], seen[:, 3, :], always)
    for d in range(DEVS):
        pos_s[d] = pos[d:d + 1].astype(jnp.int32)
        gate_s[d] = gate[d:d + 1]
    here = tabs[0]
    pos, gate = plan(here[0:1], here[1:2], here[2:3], here[3:4], each)
    pos_y[...] = pos.T
    gate_y[...] = gate.T
    own = tab_ref[...]
    pos, _ = plan(own[0:1], own[1:2], own[2:3], own[3:4], each)
    pos_x[...] = pos.T

    for c in range(2):
        got(xg, x_recv, 0, c)
        for n, b in enumerate((2, 4, 1)):
            push(xg.at[0, part[c]], xg.at[b, part[c]], x_send.at[2 * n + c], x_recv.at[b, c], st, flip(me, b))

    def pass_on(buf, ssem, rsem):
        for d, to, c_on, n in ((2, 4, 1, 6), (4, 2, 0, 7)):
            for c in range(2):
                got(buf, rsem, d, c)
            push(buf.at[d, part[c_on]], buf.at[6, part[c_on]], ssem.at[n], rsem.at[6, c_on], st, flip(me, to))
        for m, d in enumerate((2, 4)):
            for c in range(2):
                push(buf.at[d, part[c]], buf.at[d + 1, part[c]], ssem.at[8 + 2 * m + c], rsem.at[d + 1, c], st, flip(me, 1))

    def pass_last(buf, ssem, rsem):
        for c in range(2):
            got(buf, rsem, 6, c)
            push(buf.at[6, part[c]], buf.at[7, part[c]], ssem.at[12 + c], rsem.at[7, c], st, flip(me, 1))

    pass_on(dyg, dy_send, dy_recv)
    for cp in loads:
        cp.wait()

    def out_copy(d):
        return remote(out_stage.at[d], out_back.at[d], out_send.at[d], out_recv.at[d], st, flip(me, d))

    def dx_copy(d):
        return remote(dx_stage.at[d], dx_back.at[d], dxs_send.at[d], dxs_recv.at[d], other, flip(me, d))

    def local(src, dst, n):
        return pltpu.make_async_copy(src, dst, loc_sem.at[n])

    third = rows // 3

    @pl.loop(0, DEVS)
    def _(k):
        d = nth_offset(k)
        mine = col((k % 2) * rows, rows)

        @pl.when(k == 2)
        def _():
            pass_on(xg, x_send, x_recv)

        @pl.when(k == 4)
        def _():
            pass_last(dyg, dy_send, dy_recv)

        @pl.when(k == 5)
        def _():
            pass_last(xg, x_send, x_recv)

        @pl.when(d % 2 == 1)
        def _():
            for c in range(2):
                got(xg, x_recv, d, c)
                got(dyg, dy_recv, d, c)

        local(xg.at[d], xst, 0).start()

        @pl.when(k == 0)
        def _():
            local(dy_ref, dyst, 1).start()

        @pl.when(k > 0)
        def _():
            local(dyg.at[d], dyst, 1).start()

        @pl.loop(0, 3)
        def _(n):
            place = lax.broadcasted_iota(jnp.int32, (third, tok), 0) + n * third
            hit = place == pos_s[d]
            span = col(n * third, third)
            onehot[span, :] = jnp.where(hit, 1.0, 0.0).astype(BF16)
            grow[span, :] = jnp.sum(jnp.where(hit, gate_s[d], 0.0), axis=1, keepdims=True)

        local(xg.at[d], xst, 0).wait()
        local(dyg.at[d], dyst, 1).wait()

        @pl.loop(0, dim // TILE)
        def _(n):
            span = col(n * TILE, TILE)
            xr[mine, span] = mm(onehot[...], xst[:, span]).astype(BF16)
            dor[mine, span] = (grow[...] * mm(onehot[...], dyst[:, span])).astype(BF16)

        @pl.loop(0, ffn // TILE)
        def _(n):
            span = col(n * TILE, TILE)
            a = mm(xr[mine, :], wg[:, span])
            u = mm(xr[mine, :], wu[:, span])
            gh = mm(dor[mine, :], wd[span, :], NT)
            sig = jax.nn.sigmoid(a)
            act = a * sig
            hid[mine, span] = (act * u).astype(BF16)
            du[mine, span] = (gh * act).astype(BF16)
            da[mine, span] = (gh * u * sig * (1.0 + a * (1.0 - sig))).astype(BF16)

        @pl.loop(0, dim // TILE)
        def _(n):
            span = col(n * TILE, TILE)
            obuf[:, span] = mm(hid[mine, :], wd[:, span]).astype(BF16)

        @pl.when(k == 0)
        def _():
            local(obuf, out_back.at[0], 0).start()

        @pl.when(k > 0)
        def _():
            local(obuf, out_stage.at[d], 0).start()

        @pl.loop(0, dim // TILE)
        def _(n):
            span = col(n * TILE, TILE)
            dbuf[:, span] = (mm(da[mine, :], wg[span, :], NT) + mm(du[mine, :], wu[span, :], NT)).astype(BF16)

        local(dbuf, dx_stage.at[d], 1).start()
        local(obuf, out_stage.at[d], 0).wait()
        paired = (k // 2 == 1) | (k // 2 == 2)
        later = k % 2 == 1

        @pl.when((k > 0) & jnp.logical_not(paired & later))
        def _():
            out_copy(d).start()

        local(dbuf, dx_stage.at[d], 1).wait()

        @pl.when(jnp.logical_not(paired & jnp.logical_not(later)))
        def _():
            dx_copy(d).start()

        @pl.when(paired & later)
        def _():
            out_copy(d).start()
            dx_copy(nth_offset(k - 1)).start()

        @pl.when(later)
        def _():
            @pl.loop(0, dim // TILE)
            def _(m):
                over = col(m * TILE, TILE)

                @pl.loop(0, ffn // TILE)
                def _(n):
                    span = col(n * TILE, TILE)
                    accg[over, span] += mm(xr[:, over], da[:, span], TN)
                    accu[over, span] += mm(xr[:, over], du[:, span], TN)
                    accd[span, over] += mm(hid[:, span], dor[:, over], TN)

    for acc, buf in ((accg, wg), (accu, wu), (accd, wd)):
        @pl.loop(0, acc.shape[0] // 128)
        def _(n, acc=acc, buf=buf):
            span = col(n * 128, 128)
            buf[span, :] = acc[span, :].astype(BF16)
    stores = [pltpu.make_async_copy(src, dst, load_sem.at[n])
              for n, (src, dst) in enumerate(((wg, gwg_ref), (wu, gwu_ref), (wd, gwd_ref)))]
    for cp in stores:
        cp.start()

    @pl.loop(0, tok // 128)
    def _(n):
        accg[col(n * 128, 128), :] = jnp.zeros((128, ffn), F32)
        accu[col(n * 128, 128), :] = jnp.zeros((128, ffn), F32)

    @pl.loop(0, DEVS)
    def _(k):
        d = nth_offset(k)

        @pl.when(k > 0)
        def _():
            out_copy(d).wait_recv()

        dx_copy(d).wait_recv()
        local(out_back.at[d], obuf, 0).start()
        local(dx_back.at[d], dbuf, 1).start()
        local(out_back.at[d], obuf, 0).wait()
        local(dx_back.at[d], dbuf, 1).wait()

        @pl.loop(0, tok // 256)
        def _(n):
            over = col(n * 256, 256)
            place = lax.broadcasted_iota(jnp.int32, (256, rows), 1)
            lane = lax.broadcasted_iota(jnp.int32, (256, DEVS), 1) == d

            def pick(ref):
                return jnp.sum(jnp.where(lane, ref[over, :], 0.0), axis=1, keepdims=True)

            sel = jnp.where(place == pick(pos_y).astype(jnp.int32), 1.0, 0.0).astype(BF16)
            accg[over, 0:dim] += pick(gate_y) * mm(sel, obuf[...])
            sel = jnp.where(place == pick(pos_x).astype(jnp.int32), 1.0, 0.0).astype(BF16)
            accu[over, 0:dim] += mm(sel, dbuf[...])

    @pl.loop(0, tok // 128)
    def _(n):
        span = col(n * 128, 128)
        xst[span, :] = accg[span, 0:dim].astype(BF16)
        dyst[span, :] = accu[span, 0:dim].astype(BF16)

    ends = [local(xst, y_ref, 0), local(dyst, dx_ref, 1)]
    for cp in ends:
        cp.start()
    for cp in ends + stores:
        cp.wait()
    for sems, count in ((z_send, 2), (x_send, 14), (dy_send, 14)):
        for n in range(count):
            remote(xg.at[0, part[0]], xg.at[0, part[0]], sems.at[n], sems.at[n], st, me).wait_send()
    for d in range(DEVS):
        tab_copy(d).wait_send()
        dx_copy(d).wait_send()
        if d:
            out_copy(d).wait_send()


def moe_call(tab, x, dy, wg, wu, wd, cap):
    tok, dim = x.shape
    ffn = wg.shape[1]
    rows = -(-cap // 48) * 48
    sent = -(-cap // 8) * 8
    any_spec = pl.BlockSpec(memory_space=pl.ANY)
    vmem = pl.BlockSpec(memory_space=pltpu.VMEM)
    shape = jax.ShapeDtypeStruct
    out_shape = [shape((tok, dim), BF16)] * 2 + [shape(wg.shape, BF16), shape(wu.shape, BF16), shape(wd.shape, BF16)]
    out_shape += [shape((DEVS, tok, dim), BF16)] * 2 + [shape((DEVS, rows, dim), BF16)] * 4
    dma, vm = pltpu.SemaphoreType.DMA, pltpu.VMEM
    scratch = [
        vm((DEVS, 8, tok), F32), vm((DEVS, 1, tok), jnp.int32), vm((DEVS, 1, tok), F32),
        vm((tok, DEVS), F32), vm((tok, DEVS), F32), vm((tok, DEVS), F32),
        vm((dim, ffn), BF16), vm((dim, ffn), BF16), vm((ffn, dim), BF16),
        vm((dim, ffn), F32), vm((dim, ffn), F32), vm((ffn, dim), F32),
        vm((tok, dim), BF16), vm((tok, dim), BF16), vm((rows, tok), BF16), vm((rows, 1), F32),
        vm((2 * rows, dim), BF16), vm((2 * rows, dim), BF16), vm((2 * rows, ffn), BF16), vm((2 * rows, ffn), BF16), vm((2 * rows, ffn), BF16),
        vm((rows, dim), BF16), vm((rows, dim), BF16),
        dma((3,)), dma((DEVS,)), dma((DEVS,)), dma((2,)), dma((14,)), dma((14,)), dma((DEVS, 2)), dma((DEVS, 2)),
        dma((DEVS,)), dma((DEVS,)), dma((DEVS,)), dma((DEVS,)), dma((2,)),
    ]
    return pl.pallas_call(
        functools.partial(moe_kernel, rows, sent),
        out_shape=out_shape,
        in_specs=[vmem] + [any_spec] * 5,
        out_specs=[any_spec] * len(out_shape),
        scratch_shapes=scratch,
        compiler_params=pltpu.CompilerParams(collective_id=0, has_side_effects=True, vmem_limit_bytes=67043328),
    )(tab, x, dy, wg, wu, wd)


def solution(mesh):
    stages, ep_size = mesh.shape['stage'], mesh.shape['expert']
    assert stages == 2 and ep_size == DEVS
    tok_spec = P('stage', 'expert', None)
    w_spec = P('stage', 'expert', None, None)

    def device_fn(x_acts, expert_ids, gate_vals, w_gate, w_up, w_down, grad_out):
        tok, top_k = expert_ids.shape[1:]
        cap = 2 * tok * top_k // (w_gate.shape[1] * ep_size) + 1
        tab = jnp.concatenate([expert_ids[0].T.astype(F32), gate_vals[0].T, jnp.zeros((4, tok), F32)], axis=0)
        outs = moe_call(tab, x_acts[0], grad_out[0], w_gate[0, 0], w_up[0, 0], w_down[0, 0], cap)
        y, dx, gwg, gwu, gwd = outs[:5]
        return y[None], dx[None], gwg[None, None], gwu[None, None], gwd[None, None]

    return jax.shard_map(device_fn, mesh=mesh, in_specs=(tok_spec, tok_spec, tok_spec, w_spec, w_spec, w_spec, tok_spec), out_specs=(tok_spec, tok_spec, w_spec, w_spec, w_spec), check_vma=False)
```

```python
import functools

import jax
import jax.numpy as jnp
from jax import lax
from jax.experimental import pallas as pl
from jax.experimental.pallas import tpu as pltpu
from jax.sharding import PartitionSpec as P

MESH = pl.DeviceIdType.MESH
BF16 = jnp.bfloat16
F32 = jnp.float32
NN = (((1,), (0,)), ((), ()))
NT = (((1,), (1,)), ((), ()))
TN = (((0,), (0,)), ((), ()))
DEVS = 8
TILE = 512


def mm(lhs, rhs, dims=NN):
    return lax.dot_general(lhs, rhs, dims, preferred_element_type=F32)


def flip(a, b):
    out = 0
    for w in (1, 2, 4):
        p = (a // w) % 2
        q = (b // w) % 2
        out = out + w * (p + q - 2 * p * q)
    return out


def nth_offset(k):
    third, fourth = k // 3, k // 4
    return k + (third - fourth) * (1 - k // 6) - (fourth - k // 5)


def col(start, size):
    return pl.ds(pl.multiple_of(start, size), size)


def select(mask):
    return jnp.where(mask, 1.0, 0.0).astype(BF16)


def greet(st, me):
    barrier = pltpu.get_barrier_semaphore()
    for d in range(DEVS):
        if d:
            pl.semaphore_signal(barrier, inc=1, device_id=(st, flip(me, d)), device_id_type=MESH)
        pl.semaphore_signal(barrier, inc=1, device_id=(1 - st, flip(me, d)), device_id_type=MESH)
    pl.semaphore_wait(barrier, 2 * DEVS - 1)


def moe_kernel(rows, base, tab_ref, x_ref, dy_ref, wg_hbm, wu_hbm, wd_hbm,
               y_ref, dx_ref, gwg_ref, gwu_ref, gwd_ref, out_stage, dx_stage, pos_y_ref, gate_y_ref, pos_x_ref, flag_ref,
               xg, dyg, out_back, dx_back, over_own, over_peer, over_sum, over_back,
               tabs, pos_s, gate_s, shift_s, pos_y, gate_y, pos_x, over_y, over_x, flag_own, flag_peer, wg, wu, wd, accg, accu, accd, xst, dyst, onehot, grow,
               xr, dor, hid, da, du, obuf, dbuf, ovv, ovw, move,
               load_sem, tab_send, tab_recv, z_send, x_send, dy_send, x_recv, dy_recv,
               out_send, out_recv, dxs_send, dxs_recv, pair_send, pair_recv, sum_send, sum_recv, flag_sem, loc_sem):
    tok, dim = x_ref.shape
    ffn = wg_hbm.shape[1]
    half = tok // 2
    st, me = lax.axis_index('stage'), lax.axis_index('expert')
    other = 1 - st
    part = [pl.ds(0, half), pl.ds(half, half)]

    extra = rows - base
    greet(st, me)

    def remote(src, dst, ssem, rsem, stage, dev):
        return pltpu.make_async_remote_copy(src_ref=src, dst_ref=dst, send_sem=ssem, recv_sem=rsem,
                                            device_id=(stage, dev), device_id_type=MESH)

    def push(src, dst, ssem, rsem, stage, dev):
        remote(src, dst, ssem, rsem, stage, dev).start()

    def tab_copy(d):
        return remote(tab_ref, tabs.at[d], tab_send.at[d], tab_recv.at[d], other, flip(me, d))

    for d in range(DEVS):
        tab_copy(d).start()
    loads = [pltpu.make_async_copy(src, dst, load_sem.at[n])
             for n, (src, dst) in enumerate(((wg_hbm, wg), (wu_hbm, wu), (wd_hbm, wd)))]
    for c in range(2):
        push(x_ref.at[part[c]], xg.at[0, part[c]], z_send.at[c], x_recv.at[0, c], other, me)
    for c in range(2):
        for n, b in enumerate((2, 4, 1)):
            push(dy_ref.at[part[c]], dyg.at[b, part[c]], dy_send.at[2 * n + c], dy_recv.at[b, c], st, flip(me, b))
    for cp in loads:
        cp.start()

    def got(buf, sems, d, c):
        remote(buf.at[d, part[c]], buf.at[d, part[c]], z_send.at[0], sems.at[d, c], st, me).wait_recv()

    @pl.loop(0, tok // 128)
    def _(n):
        accg[col(n * 128, 128), :] = jnp.zeros((128, ffn), F32)
        accu[col(n * 128, 128), :] = jnp.zeros((128, ffn), F32)

    @pl.loop(0, ffn // 128)
    def _(n):
        accd[col(n * 128, 128), :] = jnp.zeros((128, dim), F32)

    xst[...] = jnp.where(lax.broadcasted_iota(jnp.int32, (tok, tok), 0) < lax.broadcasted_iota(jnp.int32, (tok, tok), 1),
                         1.0, 0.0).astype(BF16)
    for d in range(DEVS):
        tab_copy(d).wait_recv()

    sub = lax.broadcasted_iota(jnp.int32, (DEVS, tok), 0)
    each = sub.astype(F32)
    sub_col = lax.broadcasted_iota(jnp.int32, (DEVS, 1), 0)

    def earlier(named):
        return jnp.where(named, mm(select(named), xst[...]), -1.0)

    def spilled(named):
        past = jnp.maximum(jnp.sum(jnp.where(named, 1.0, 0.0), axis=1, keepdims=True) - base, 0.0)
        start, total = jnp.zeros((DEVS, 1), F32), jnp.zeros((1, 1), F32)
        for e in range(DEVS):
            start = jnp.where(sub_col == e, total, start)
            total = total + past[e:e + 1]
        return start, total

    def source_tables(tab):
        first, second = tab[0:1] == each, tab[1:2] == each
        named = jnp.logical_or(first, second)
        pos = earlier(named)
        gate = jnp.where(first, tab[2:3], jnp.where(second, tab[3:4], 0.0))
        start, _ = spilled(named)
        shared = jnp.where(pos >= base, pos - base + start + 1.0, 0.0)
        place = [jnp.sum(jnp.where(which, shared, 0.0), axis=0, keepdims=True) - 1.0 for which in (first, second)]
        over = jnp.where(sub == 0, place[0], jnp.where(sub == 1, place[1], jnp.where(sub == 2, tab[2:3], tab[3:4])))
        return pos.T, gate.T, over.T

    seen = tabs[...]
    me_f = me.astype(F32)
    first, second = seen[:, 0, :] == me_f, seen[:, 1, :] == me_f
    pos = earlier(jnp.logical_or(first, second))
    gate = jnp.where(first, seen[:, 2, :], jnp.where(second, seen[:, 3, :], 0.0))
    most = jnp.zeros((1, 1), F32)
    for d in range(DEVS):
        pos_s[d] = pos[d:d + 1].astype(jnp.int32)
        gate_s[d] = gate[d:d + 1]
        start, total = spilled(jnp.logical_or(seen[d, 0:1] == each, seen[d, 1:2] == each))
        mine = jnp.sum(jnp.where(sub_col == me, start, 0.0), axis=0, keepdims=True)
        shift_s[d] = jnp.broadcast_to(mine, (1, 128)).astype(jnp.int32)
        most = jnp.maximum(most, total)
    flag_own[...] = jnp.broadcast_to(jnp.where(most > extra, 1.0, 0.0), (8, 128))
    pos_y[...], gate_y[...], over_y[...] = source_tables(tabs[0])
    pos_x[...], _, over_x[...] = source_tables(tab_ref[...])

    for c in range(2):
        got(xg, x_recv, 0, c)
        for n, b in enumerate((2, 4, 1)):
            push(xg.at[0, part[c]], xg.at[b, part[c]], x_send.at[2 * n + c], x_recv.at[b, c], st, flip(me, b))

    def pass_on(buf, ssem, rsem):
        for d, to, c_on, n in ((2, 4, 1, 6), (4, 2, 0, 7)):
            for c in range(2):
                got(buf, rsem, d, c)
            push(buf.at[d, part[c_on]], buf.at[6, part[c_on]], ssem.at[n], rsem.at[6, c_on], st, flip(me, to))
        for m, d in enumerate((2, 4)):
            for c in range(2):
                push(buf.at[d, part[c]], buf.at[d + 1, part[c]], ssem.at[8 + 2 * m + c], rsem.at[d + 1, c], st, flip(me, 1))

    def pass_last(buf, ssem, rsem):
        for c in range(2):
            got(buf, rsem, 6, c)
            push(buf.at[6, part[c]], buf.at[7, part[c]], ssem.at[12 + c], rsem.at[7, c], st, flip(me, 1))

    pass_on(dyg, dy_send, dy_recv)
    for cp in loads:
        cp.wait()

    def out_copy(d):
        return remote(out_stage.at[d, pl.ds(0, base)], out_back.at[d], out_send.at[d], out_recv.at[d], st, flip(me, d))

    def dx_copy(d):
        return remote(dx_stage.at[d, pl.ds(0, base)], dx_back.at[d], dxs_send.at[d], dxs_recv.at[d], other, flip(me, d))

    def local(src, dst, n):
        return pltpu.make_async_copy(src, dst, loc_sem.at[n])

    def pair_copy(t, d):
        return remote(over_own.at[t, d], over_peer.at[t, d // 2], pair_send.at[t, d // 2], pair_recv.at[t, d // 2], st, flip(me, 1))

    def sum_copy(t, j):
        return remote(over_sum.at[t, j], over_back.at[t, j], sum_send.at[t, j], sum_recv.at[t, j], other if t else st, flip(me, 2 * j))

    def merge(j):
        for t in range(2):
            pair_copy(t, 2 * j).wait_recv()
            local(over_own.at[t, 2 * j], ovv.at[t], t).start()
            local(over_peer.at[t, j], ovw.at[t], 2 + t).start()
        for t in range(2):
            local(over_own.at[t, 2 * j], ovv.at[t], t).wait()
            local(over_peer.at[t, j], ovw.at[t], 2 + t).wait()
            ovv[t] = (ovv[t].astype(F32) + ovw[t].astype(F32)).astype(BF16)
            to = over_back if t == 0 and j == 0 else over_sum
            local(ovv.at[t], to.at[t, j], t).start()
        for t in range(2):
            local(ovv.at[t], over_sum.at[t, j], t).wait()
            if t or j:
                sum_copy(t, j).start()

    third = rows // 3

    @pl.loop(0, DEVS)
    def _(k):
        d = nth_offset(k)
        mine = col((k % 2) * rows, rows)

        @pl.when(k == 2)
        def _():
            pass_on(xg, x_send, x_recv)

        @pl.when(k == 4)
        def _():
            pass_last(dyg, dy_send, dy_recv)

        @pl.when(k == 5)
        def _():
            pass_last(xg, x_send, x_recv)

        @pl.when(d % 2 == 1)
        def _():
            for c in range(2):
                got(xg, x_recv, d, c)
                got(dyg, dy_recv, d, c)

        local(xg.at[d], xst, 0).start()

        @pl.when(k == 0)
        def _():
            local(dy_ref, dyst, 1).start()

        @pl.when(k > 0)
        def _():
            local(dyg.at[d], dyst, 1).start()

        @pl.loop(0, 3)
        def _(n):
            place = lax.broadcasted_iota(jnp.int32, (third, tok), 0) + n * third
            hit = place == pos_s[d]
            span = col(n * third, third)
            onehot[span, :] = jnp.where(hit, 1.0, 0.0).astype(BF16)
            grow[span, :] = jnp.sum(jnp.where(hit, gate_s[d], 0.0), axis=1, keepdims=True)

        move[...] = select(lax.broadcasted_iota(jnp.int32, (extra, extra), 0)
                           == lax.broadcasted_iota(jnp.int32, (extra, extra), 1) + shift_s[d][:, 0:1])
        local(xg.at[d], xst, 0).wait()
        local(dyg.at[d], dyst, 1).wait()

        @pl.loop(0, dim // TILE)
        def _(n):
            span = col(n * TILE, TILE)
            xr[mine, span] = mm(onehot[...], xst[:, span]).astype(BF16)
            dor[mine, span] = (grow[...] * mm(onehot[...], dyst[:, span])).astype(BF16)

        @pl.loop(0, ffn // TILE)
        def _(n):
            span = col(n * TILE, TILE)
            a = mm(xr[mine, :], wg[:, span])
            u = mm(xr[mine, :], wu[:, span])
            gh = mm(dor[mine, :], wd[span, :], NT)
            sig = jax.nn.sigmoid(a)
            act = a * sig
            hid[mine, span] = (act * u).astype(BF16)
            du[mine, span] = (gh * act).astype(BF16)
            da[mine, span] = (gh * u * sig * (1.0 + a * (1.0 - sig))).astype(BF16)

        @pl.loop(0, dim // TILE)
        def _(n):
            span = col(n * TILE, TILE)
            obuf[:, span] = mm(hid[mine, :], wd[:, span]).astype(BF16)

        local(obuf, out_stage.at[d], 0).start()
        ovv[0] = mm(move[...], obuf[base:, :]).astype(BF16)
        local(ovv.at[0], over_own.at[0, d], 2).start()

        @pl.loop(0, dim // TILE)
        def _(n):
            span = col(n * TILE, TILE)
            dbuf[:, span] = (mm(da[mine, :], wg[span, :], NT) + mm(du[mine, :], wu[span, :], NT)).astype(BF16)

        local(dbuf, dx_stage.at[d], 1).start()
        ovv[1] = mm(move[...], dbuf[base:, :]).astype(BF16)
        local(ovv.at[1], over_own.at[1, d], 3).start()
        local(obuf, out_stage.at[d], 0).wait()
        for t in range(2):
            local(ovv.at[t], over_own.at[t, d], 2 + t).wait()

        @pl.when(d % 2 == 1)
        def _():
            for t in range(2):
                pair_copy(t, d).start()

        paired = (k // 2 == 1) | (k // 2 == 2)
        later = k % 2 == 1

        @pl.when((k > 0) & jnp.logical_not(paired & later))
        def _():
            out_copy(d).start()

        local(dbuf, dx_stage.at[d], 1).wait()

        @pl.when(jnp.logical_not(paired & jnp.logical_not(later)))
        def _():
            dx_copy(d).start()

        @pl.when(paired & later)
        def _():
            out_copy(d).start()
            dx_copy(nth_offset(k - 1)).start()

        @pl.when(k == DEVS - 1)
        def _():
            merge(3)

        @pl.when(later)
        def _():
            @pl.loop(0, dim // TILE)
            def _(m):
                over = col(m * TILE, TILE)

                @pl.loop(0, ffn // TILE)
                def _(n):
                    span = col(n * TILE, TILE)
                    accg[over, span] += mm(xr[:, over], da[:, span], TN)
                    accu[over, span] += mm(xr[:, over], du[:, span], TN)
                    accd[span, over] += mm(hid[:, span], dor[:, over], TN)

        @pl.when(k == 3)
        def _():
            merge(0)

        @pl.when(k == 5)
        def _():
            merge(1)
            merge(2)

    flag_copy = remote(flag_own, flag_peer, flag_sem.at[0], flag_sem.at[1], other, me)
    flag_copy.start()

    for acc, buf in ((accg, wg), (accu, wu), (accd, wd)):
        @pl.loop(0, acc.shape[0] // 128)
        def _(n, acc=acc, buf=buf):
            span = col(n * 128, 128)
            buf[span, :] = acc[span, :].astype(BF16)
    stores = [pltpu.make_async_copy(src, dst, load_sem.at[n])
              for n, (src, dst) in enumerate(((wg, gwg_ref), (wu, gwu_ref), (wd, gwd_ref)))]
    for cp in stores:
        cp.start()

    @pl.loop(0, tok // 128)
    def _(n):
        accg[col(n * 128, 128), :] = jnp.zeros((128, ffn), F32)
        accu[col(n * 128, 128), :] = jnp.zeros((128, ffn), F32)

    @pl.loop(0, DEVS)
    def _(k):
        d = nth_offset(k)

        @pl.when(k == 0)
        def _():
            local(out_stage.at[0, pl.ds(0, base)], obuf.at[pl.ds(0, base)], 0).start()

        @pl.when(k > 0)
        def _():
            out_copy(d).wait_recv()
            local(out_back.at[d], obuf.at[pl.ds(0, base)], 0).start()

        dx_copy(d).wait_recv()
        local(dx_back.at[d], dbuf.at[pl.ds(0, base)], 1).start()
        local(out_back.at[d], obuf.at[pl.ds(0, base)], 0).wait()
        local(dx_back.at[d], dbuf.at[pl.ds(0, base)], 1).wait()

        @pl.loop(0, tok // 256)
        def _(n):
            over = col(n * 256, 256)
            place = lax.broadcasted_iota(jnp.int32, (256, base), 1)
            lane = lax.broadcasted_iota(jnp.int32, (256, DEVS), 1) == flip(me, d)

            def pick(ref):
                return jnp.sum(jnp.where(lane, ref[over, :], 0.0), axis=1, keepdims=True)

            accg[over, 0:dim] += pick(gate_y) * mm(select(place == pick(pos_y).astype(jnp.int32)), obuf[0:base, :])
            accu[over, 0:dim] += mm(select(place == pick(pos_x).astype(jnp.int32)), dbuf[0:base, :])

    for j in range(4):
        for t in range(2):
            if t or j:
                sum_copy(t, j).wait_recv()
            local(over_back.at[t, j], ovw.at[t] if j else ovv.at[t], t).start()
        for t in range(2):
            local(over_back.at[t, j], ovw.at[t] if j else ovv.at[t], t).wait()
            if j:
                ovv[t] = (ovv[t].astype(F32) + ovw[t].astype(F32)).astype(BF16)

    @pl.loop(0, tok // 256)
    def _(n):
        over = col(n * 256, 256)
        place = lax.broadcasted_iota(jnp.int32, (256, extra), 1)
        at_y, at_x = over_y[over, :], over_x[over, :]

        def chosen(tab, c):
            return place == tab[:, c:c + 1].astype(jnp.int32)

        for c in range(2):
            accg[over, 0:dim] += at_y[:, 2 + c:3 + c] * mm(select(chosen(at_y, c)), ovv[0])
        accu[over, 0:dim] += mm(select(jnp.logical_or(chosen(at_x, 0), chosen(at_x, 1))), ovv[1])

    @pl.loop(0, tok // 128)
    def _(n):
        span = col(n * 128, 128)
        xst[span, :] = accg[span, 0:dim].astype(BF16)
        dyst[span, :] = accu[span, 0:dim].astype(BF16)

    flag_copy.wait()
    flag_own[...] = jnp.maximum(flag_own[...], flag_peer[...])
    ends = [local(xst, y_ref, 0), local(dyst, dx_ref, 1), local(flag_own, flag_ref, 2), local(pos_y, pos_y_ref, 3),
            local(gate_y, gate_y_ref, 4), local(pos_x, pos_x_ref, 5)]
    for cp in ends:
        cp.start()
    for cp in ends + stores:
        cp.wait()
    for sems, count in ((z_send, 2), (x_send, 14), (dy_send, 14)):
        for n in range(count):
            remote(xg.at[0, part[0]], xg.at[0, part[0]], sems.at[n], sems.at[n], st, me).wait_send()
    for d in range(DEVS):
        tab_copy(d).wait_send()
        dx_copy(d).wait_send()
        if d:
            out_copy(d).wait_send()
    for j in range(4):
        for t in range(2):
            pair_copy(t, 2 * j).wait_send()
            if t or j:
                sum_copy(t, j).wait_send()


def return_kernel(out_stage, dx_stage, pos_y, gate_y, pos_x, y_ref, dx_ref, out_back, dx_back,
                  acc_y, acc_x, obuf, dbuf, ybuf, xbuf, out_send, out_recv, dxs_send, dxs_recv, loc_sem):
    tok, dim = y_ref.shape
    rows = out_stage.shape[1]
    st, me = lax.axis_index('stage'), lax.axis_index('expert')
    greet(st, me)

    def out_copy(d):
        return pltpu.make_async_remote_copy(src_ref=out_stage.at[d], dst_ref=out_back.at[d], send_sem=out_send.at[d],
                                            recv_sem=out_recv.at[d], device_id=(st, flip(me, d)), device_id_type=MESH)

    def dx_copy(d):
        return pltpu.make_async_remote_copy(src_ref=dx_stage.at[d], dst_ref=dx_back.at[d], send_sem=dxs_send.at[d],
                                            recv_sem=dxs_recv.at[d], device_id=(1 - st, flip(me, d)), device_id_type=MESH)

    def local(src, dst, n):
        return pltpu.make_async_copy(src, dst, loc_sem.at[n])

    for d in range(DEVS):
        dx_copy(d).start()
        if d:
            out_copy(d).start()
    acc_y[...] = jnp.zeros_like(acc_y)
    acc_x[...] = jnp.zeros_like(acc_x)

    @pl.loop(0, DEVS)
    def _(d):
        @pl.when(d == 0)
        def _():
            local(out_stage.at[0], obuf, 0).start()

        @pl.when(d > 0)
        def _():
            out_copy(d).wait_recv()
            local(out_back.at[d], obuf, 0).start()

        dx_copy(d).wait_recv()
        local(dx_back.at[d], dbuf, 1).start()
        local(out_back.at[d], obuf, 0).wait()
        local(dx_back.at[d], dbuf, 1).wait()

        @pl.loop(0, tok // 256)
        def _(n):
            over = col(n * 256, 256)
            place = lax.broadcasted_iota(jnp.int32, (256, rows), 1)
            lane = lax.broadcasted_iota(jnp.int32, (256, DEVS), 1) == flip(me, d)

            def pick(ref):
                return jnp.sum(jnp.where(lane, ref[over, :], 0.0), axis=1, keepdims=True)

            acc_y[over, :] += pick(gate_y) * mm(select(place == pick(pos_y).astype(jnp.int32)), obuf[...])
            acc_x[over, :] += mm(select(place == pick(pos_x).astype(jnp.int32)), dbuf[...])

    ybuf[...] = acc_y[...].astype(BF16)
    xbuf[...] = acc_x[...].astype(BF16)
    ends = [local(ybuf, y_ref, 0), local(xbuf, dx_ref, 1)]
    for cp in ends:
        cp.start()
    for cp in ends:
        cp.wait()
    for d in range(DEVS):
        dx_copy(d).wait_send()
        if d:
            out_copy(d).wait_send()


def return_call(out_stage, dx_stage, pos_y, gate_y, pos_x):
    rows, dim = out_stage.shape[1:]
    tok = pos_y.shape[0]
    any_spec = pl.BlockSpec(memory_space=pl.ANY)
    vmem = pl.BlockSpec(memory_space=pltpu.VMEM)
    dma, vm, shape = pltpu.SemaphoreType.DMA, pltpu.VMEM, jax.ShapeDtypeStruct
    outs = pl.pallas_call(
        return_kernel,
        out_shape=[shape((tok, dim), BF16)] * 2 + [shape(out_stage.shape, BF16)] * 2,
        in_specs=[any_spec] * 2 + [vmem] * 3,
        out_specs=[any_spec] * 4,
        scratch_shapes=[vm((tok, dim), F32)] * 2 + [vm((rows, dim), BF16)] * 2 + [vm((tok, dim), BF16)] * 2
        + [dma((DEVS,))] * 4 + [dma((2,))],
        compiler_params=pltpu.CompilerParams(collective_id=1, has_side_effects=True),
    )(out_stage, dx_stage, pos_y, gate_y, pos_x)
    return outs[0], outs[1]


def moe_call(tab, x, dy, wg, wu, wd, cap, mean):
    tok, dim = x.shape
    ffn = wg.shape[1]
    rows = -(-cap // 48) * 48
    base = mean // 32 * 28
    extra = rows - base
    any_spec = pl.BlockSpec(memory_space=pl.ANY)
    vmem = pl.BlockSpec(memory_space=pltpu.VMEM)
    shape = jax.ShapeDtypeStruct
    out_shape = [shape((tok, dim), BF16)] * 2 + [shape(wg.shape, BF16), shape(wu.shape, BF16), shape(wd.shape, BF16)]
    out_shape += [shape((DEVS, rows, dim), BF16)] * 2 + [shape((tok, DEVS), F32)] * 3 + [shape((8, 128), F32)]
    out_shape += [shape((DEVS, tok, dim), BF16)] * 2 + [shape((DEVS, base, dim), BF16)] * 2
    out_shape += [shape((2, DEVS, extra, dim), BF16)] + [shape((2, 4, extra, dim), BF16)] * 3
    dma, vm = pltpu.SemaphoreType.DMA, pltpu.VMEM
    scratch = [
        vm((DEVS, 8, tok), F32), vm((DEVS, 1, tok), jnp.int32), vm((DEVS, 1, tok), F32), vm((DEVS, 1, 128), jnp.int32),
        vm((tok, DEVS), F32), vm((tok, DEVS), F32), vm((tok, DEVS), F32), vm((tok, DEVS), F32), vm((tok, DEVS), F32),
        vm((8, 128), F32), vm((8, 128), F32),
        vm((dim, ffn), BF16), vm((dim, ffn), BF16), vm((ffn, dim), BF16),
        vm((dim, ffn), F32), vm((dim, ffn), F32), vm((ffn, dim), F32),
        vm((tok, dim), BF16), vm((tok, dim), BF16), vm((rows, tok), BF16), vm((rows, 1), F32),
        vm((2 * rows, dim), BF16), vm((2 * rows, dim), BF16), vm((2 * rows, ffn), BF16), vm((2 * rows, ffn), BF16), vm((2 * rows, ffn), BF16),
        vm((rows, dim), BF16), vm((rows, dim), BF16), vm((2, extra, dim), BF16), vm((2, extra, dim), BF16), vm((extra, extra), BF16),
        dma((3,)), dma((DEVS,)), dma((DEVS,)), dma((2,)), dma((14,)), dma((14,)), dma((DEVS, 2)), dma((DEVS, 2)),
        dma((DEVS,)), dma((DEVS,)), dma((DEVS,)), dma((DEVS,)), dma((2, 4)), dma((2, 4)), dma((2, 4)), dma((2, 4)), dma((2,)), dma((6,)),
    ]
    return pl.pallas_call(
        functools.partial(moe_kernel, rows, base),
        out_shape=out_shape,
        in_specs=[vmem] + [any_spec] * 5,
        out_specs=[any_spec] * len(out_shape),
        scratch_shapes=scratch,
        compiler_params=pltpu.CompilerParams(collective_id=0, has_side_effects=True, vmem_limit_bytes=67043328),
    )(tab, x, dy, wg, wu, wd)


def solution(mesh):
    stages, ep_size = mesh.shape['stage'], mesh.shape['expert']
    assert stages == 2 and ep_size == DEVS
    tok_spec = P('stage', 'expert', None)
    w_spec = P('stage', 'expert', None, None)

    def device_fn(x_acts, expert_ids, gate_vals, w_gate, w_up, w_down, grad_out):
        tok, top_k = expert_ids.shape[1:]
        cap = 2 * tok * top_k // (w_gate.shape[1] * ep_size) + 1
        tab = jnp.concatenate([expert_ids[0].T.astype(F32), gate_vals[0].T, jnp.zeros((4, tok), F32)], axis=0)
        outs = moe_call(tab, x_acts[0], grad_out[0], w_gate[0, 0], w_up[0, 0], w_down[0, 0], cap, tok * top_k // ep_size)
        y, dx, gwg, gwu, gwd = outs[:5]
        y, dx = lax.cond(outs[10][0, 0] > 0, return_call, lambda *_: (y, dx), *outs[5:10])
        return y[None], dx[None], gwg[None, None], gwu[None, None], gwd[None, None]

    return jax.shard_map(device_fn, mesh=mesh, in_specs=(tok_spec, tok_spec, tok_spec, w_spec, w_spec, w_spec, tok_spec), out_specs=(tok_spec, tok_spec, w_spec, w_spec, w_spec), check_vma=False)
```

```python
import functools

import jax
import jax.numpy as jnp
from jax import lax
from jax.experimental import pallas as pl
from jax.experimental.pallas import tpu as pltpu
from jax.sharding import PartitionSpec as P

MESH = pl.DeviceIdType.MESH
BF16 = jnp.bfloat16
F32 = jnp.float32
NN = (((1,), (0,)), ((), ()))
NT = (((1,), (1,)), ((), ()))
TN = (((0,), (0,)), ((), ()))
DEVS = 8
TILE = 512


def mm(lhs, rhs, dims=NN):
    return lax.dot_general(lhs, rhs, dims, preferred_element_type=F32)


def flip(a, b):
    out = 0
    for w in (1, 2, 4):
        p = (a // w) % 2
        q = (b // w) % 2
        out = out + w * (p + q - 2 * p * q)
    return out


def nth_offset(k):
    third, fourth = k // 3, k // 4
    return k + (third - fourth) * (1 - k // 6) - (fourth - k // 5)


def col(start, size):
    return pl.ds(pl.multiple_of(start, size), size)


def select(mask):
    return jnp.where(mask, 1.0, 0.0).astype(BF16)


def greet(st, me):
    barrier = pltpu.get_barrier_semaphore()
    for d in range(DEVS):
        if d:
            pl.semaphore_signal(barrier, inc=1, device_id=(st, flip(me, d)), device_id_type=MESH)
        pl.semaphore_signal(barrier, inc=1, device_id=(1 - st, flip(me, d)), device_id_type=MESH)
    pl.semaphore_wait(barrier, 2 * DEVS - 1)


def moe_kernel(rows, base, tab_ref, x_ref, dy_ref, wg_hbm, wu_hbm, wd_hbm,
               y_ref, dx_ref, gwg_ref, gwu_ref, gwd_ref, out_stage, dx_stage, pos_y_ref, gate_y_ref, pos_x_ref, flag_ref,
               xg, dyg, out_back, dx_back, over_own, over_peer, over_sum, over_back,
               keep_x, keep_do, keep_h, keep_da, keep_du,
               tabs, pos_s, gate_s, shift_s, pos_y, gate_y, pos_x, over_y, over_x, flag_own, flag_peer, wg, wu, wd, accg, accu, accd, xst, dyst, onehot, grow,
               xr, dor, hid, da, du, obuf, dbuf, ovv, ova, ovw, move,
               load_sem, tab_send, tab_recv, z_send, x_send, dy_send, x_recv, dy_recv,
               out_send, out_recv, dxs_send, dxs_recv, pair_send, pair_recv, sum_send, sum_recv, flag_sem, loc_sem, keep_sem):
    tok, dim = x_ref.shape
    ffn = wg_hbm.shape[1]
    half = tok // 2
    st, me = lax.axis_index('stage'), lax.axis_index('expert')
    other = 1 - st
    core = me % 2
    part = [pl.ds(0, half), pl.ds(half, half)]

    extra = rows - base
    greet(st, me)

    def remote(src, dst, ssem, rsem, stage, dev):
        return pltpu.make_async_remote_copy(src_ref=src, dst_ref=dst, send_sem=ssem, recv_sem=rsem,
                                            device_id=(stage, dev), device_id_type=MESH)

    def push(src, dst, ssem, rsem, stage, dev):
        remote(src, dst, ssem, rsem, stage, dev).start()

    def tab_copy(d):
        return remote(tab_ref, tabs.at[d], tab_send.at[d], tab_recv.at[d], other, flip(me, d))

    for d in range(DEVS):
        tab_copy(d).start()
    loads = [pltpu.make_async_copy(src, dst, load_sem.at[n])
             for n, (src, dst) in enumerate(((wg_hbm, wg), (wu_hbm, wu), (wd_hbm, wd)))]
    def send_x():
        for c in range(2):
            push(x_ref.at[part[c]], xg.at[0, part[c]], z_send.at[c], x_recv.at[0, c], other, me)

    def send_dy(targets):
        for n, b in targets:
            for c in range(2):
                push(dy_ref.at[part[c]], dyg.at[b, part[c]], dy_send.at[2 * n + c], dy_recv.at[b, c], st, flip(me, b))

    @pl.when(core == 0)
    def _():
        send_x()
        send_dy(((0, 2), (1, 4)))

    send_dy(((2, 1),))
    for cp in loads:
        cp.start()

    def got(buf, sems, d, c):
        remote(buf.at[d, part[c]], buf.at[d, part[c]], z_send.at[0], sems.at[d, c], st, me).wait_recv()

    @pl.loop(0, tok // 128)
    def _(n):
        accg[col(n * 128, 128), :] = jnp.zeros((128, ffn), F32)
        accu[col(n * 128, 128), :] = jnp.zeros((128, ffn), F32)

    @pl.loop(0, ffn // 128)
    def _(n):
        accd[col(n * 128, 128), :] = jnp.zeros((128, dim), F32)

    xst[...] = jnp.where(lax.broadcasted_iota(jnp.int32, (tok, tok), 0) < lax.broadcasted_iota(jnp.int32, (tok, tok), 1),
                         1.0, 0.0).astype(BF16)
    for d in range(DEVS):
        tab_copy(d).wait_recv()

    sub = lax.broadcasted_iota(jnp.int32, (DEVS, tok), 0)
    each = sub.astype(F32)
    sub_col = lax.broadcasted_iota(jnp.int32, (DEVS, 1), 0)

    def earlier(named):
        return jnp.where(named, mm(select(named), xst[...]), -1.0)

    def spilled(named):
        past = jnp.maximum(jnp.sum(jnp.where(named, 1.0, 0.0), axis=1, keepdims=True) - base, 0.0)
        start, total = jnp.zeros((DEVS, 1), F32), jnp.zeros((1, 1), F32)
        for e in range(DEVS):
            start = jnp.where(sub_col == e, total, start)
            total = total + past[e:e + 1]
        return start, total

    def source_tables(tab):
        first, second = tab[0:1] == each, tab[1:2] == each
        named = jnp.logical_or(first, second)
        pos = earlier(named)
        gate = jnp.where(first, tab[2:3], jnp.where(second, tab[3:4], 0.0))
        start, _ = spilled(named)
        shared = jnp.where(pos >= base, pos - base + start + 1.0, 0.0)
        place = [jnp.sum(jnp.where(which, shared, 0.0), axis=0, keepdims=True) - 1.0 for which in (first, second)]
        over = jnp.where(sub == 0, place[0], jnp.where(sub == 1, place[1], jnp.where(sub == 2, tab[2:3], tab[3:4])))
        return pos.T, gate.T, over.T

    seen = tabs[...]
    me_f = me.astype(F32)
    first, second = seen[:, 0, :] == me_f, seen[:, 1, :] == me_f
    pos = earlier(jnp.logical_or(first, second))
    gate = jnp.where(first, seen[:, 2, :], jnp.where(second, seen[:, 3, :], 0.0))
    most = jnp.zeros((1, 1), F32)
    for d in range(DEVS):
        pos_s[d] = pos[d:d + 1].astype(jnp.int32)
        gate_s[d] = gate[d:d + 1]
        start, total = spilled(jnp.logical_or(seen[d, 0:1] == each, seen[d, 1:2] == each))
        mine = jnp.sum(jnp.where(sub_col == me, start, 0.0), axis=0, keepdims=True)
        shift_s[d] = jnp.broadcast_to(mine, (1, 128)).astype(jnp.int32)
        most = jnp.maximum(most, total)
    flag_own[...] = jnp.broadcast_to(jnp.where(most > extra, 1.0, 0.0), (8, 128))
    pos_y[...], gate_y[...], over_y[...] = source_tables(tabs[0])
    pos_x[...], _, over_x[...] = source_tables(tab_ref[...])

    def spread_x():
        for c in range(2):
            got(xg, x_recv, 0, c)
            for n, b in enumerate((2, 4, 1)):
                push(xg.at[0, part[c]], xg.at[b, part[c]], x_send.at[2 * n + c], x_recv.at[b, c], st, flip(me, b))

    def pass_on(buf, ssem, rsem):
        for d, to, c_on, n in ((2, 4, 1, 6), (4, 2, 0, 7)):
            for c in range(2):
                got(buf, rsem, d, c)
            push(buf.at[d, part[c_on]], buf.at[6, part[c_on]], ssem.at[n], rsem.at[6, c_on], st, flip(me, to))
        for m, d in enumerate((2, 4)):
            for c in range(2):
                push(buf.at[d, part[c]], buf.at[d + 1, part[c]], ssem.at[8 + 2 * m + c], rsem.at[d + 1, c], st, flip(me, 1))

    def pass_last(buf, ssem, rsem):
        for c in range(2):
            got(buf, rsem, 6, c)
            push(buf.at[6, part[c]], buf.at[7, part[c]], ssem.at[12 + c], rsem.at[7, c], st, flip(me, 1))

    def order(k):
        near = nth_offset(k)
        return near + core * (1 - 2 * (near % 2))

    def fetch(k):
        d = order(k)

        @pl.when((d % 2 == 1) & (k > 0))
        def _():
            for c in range(2):
                got(xg, x_recv, d, c)

        @pl.when(d % 2 == 1)
        def _():
            for c in range(2):
                got(dyg, dy_recv, d, c)

        pltpu.make_async_copy(xg.at[d], xst, loc_sem.at[4]).start()

        @pl.when(d == 0)
        def _():
            pltpu.make_async_copy(dy_ref, dyst, loc_sem.at[5]).start()

        @pl.when(d > 0)
        def _():
            pltpu.make_async_copy(dyg.at[d], dyst, loc_sem.at[5]).start()

    for cp in loads:
        cp.wait()

    @pl.when(core == 0)
    def _():
        spread_x()
        pass_on(dyg, dy_send, dy_recv)

    @pl.when(core == 1)
    def _():
        for c in range(2):
            got(xg, x_recv, 1, c)
        send_x()
        send_dy(((0, 2), (1, 4)))

    def out_copy(d):
        return remote(out_stage.at[d, pl.ds(0, base)], out_back.at[d], out_send.at[d], out_recv.at[d], st, flip(me, d))

    def dx_copy(d):
        return remote(dx_stage.at[d, pl.ds(0, base)], dx_back.at[d], dxs_send.at[d], dxs_recv.at[d], other, flip(me, d))

    def local(src, dst, n):
        return pltpu.make_async_copy(src, dst, loc_sem.at[n])

    def pair_copy(t, d):
        return remote(over_own.at[t, d], over_peer.at[t, d // 2], pair_send.at[t, d // 2], pair_recv.at[t, d // 2], st, flip(me, 1))

    def sum_copy(t, j):
        return remote(over_sum.at[t, j], over_back.at[t, j], sum_send.at[t, j], sum_recv.at[t, j], other if t else st, flip(me, 2 * j))

    def merge_load(j):
        for t in range(2):
            pair_copy(t, 2 * j).wait_recv()
            local(over_own.at[t, 2 * j], ova.at[t], 6 + t).start()
            local(over_peer.at[t, j], ovw.at[t], 8 + t).start()

    def merge_add(j):
        for t in range(2):
            local(over_own.at[t, 2 * j], ova.at[t], 6 + t).wait()
            local(over_peer.at[t, j], ovw.at[t], 8 + t).wait()
            ova[t] = (ova[t].astype(F32) + ovw[t].astype(F32)).astype(BF16)
            to = over_back if t == 0 and j == 0 else over_sum
            local(ova.at[t], to.at[t, j], 6 + t).start()

    def merge_send(j):
        for t in range(2):
            local(ova.at[t], over_sum.at[t, j], 6 + t).wait()
            if t or j:
                sum_copy(t, j).start()

    def merges(k, step):
        for j, (low, high) in enumerate(((2, 3), (3, 5), (4, 6), (7, 8))):
            @pl.when(k == low + core * (high - low))
            def _(j=j):
                step(j)

    kept = ((xr, keep_x), (dor, keep_do), (hid, keep_h), (da, keep_da), (du, keep_du))

    def region(k):
        return col((k % 2) * rows, rows)

    def keep(k):
        return [pltpu.make_async_copy(buf.at[region(k)], hbm.at[k - 3], keep_sem.at[5 * (k % 2) + n])
                for n, (buf, hbm) in enumerate(kept)]

    def bring(k):
        return [pltpu.make_async_copy(hbm.at[k - 3], buf.at[region(k + 1)], keep_sem.at[5 * ((k + 1) % 2) + n])
                for n, (buf, hbm) in enumerate(kept)]

    def weight_grads(span_k, middle):
        @pl.loop(0, dim // TILE)
        def _(m):
            over = col(m * TILE, TILE)

            @pl.when(m == 1)
            def _():
                middle()

            @pl.loop(0, ffn // TILE)
            def _(n):
                span = col(n * TILE, TILE)
                accg[over, span] += mm(xr[span_k, over], da[span_k, span], TN)
                accu[over, span] += mm(xr[span_k, over], du[span_k, span], TN)
                accd[span, over] += mm(hid[span_k, span], dor[span_k, over], TN)

    def send_back(k):
        d = order(k)
        local(obuf, out_stage.at[d], 0).wait()
        local(dbuf, dx_stage.at[d], 1).wait()
        for t in range(2):
            local(ovv.at[t], over_own.at[t, d], 2 + t).wait()
        paired = (k // 2 == 1) | (k // 2 == 2)
        later = k % 2 == 1

        @pl.when((d > 0) & jnp.logical_not(paired & later))
        def _():
            out_copy(d).start()

        @pl.when(jnp.logical_not(paired & jnp.logical_not(later)))
        def _():
            dx_copy(d).start()

        @pl.when(paired & later)
        def _():
            out_copy(d).start()
            dx_copy(order(k - 1)).start()

        @pl.when(d % 2 == 1)
        def _():
            for t in range(2):
                pair_copy(t, d).start()

    third = rows // 3

    @pl.loop(0, DEVS)
    def _(k):
        d = order(k)
        mine = region(k)

        @pl.when((k == 1) & (core == 1))
        def _():
            spread_x()

        @pl.when((k == 2) & (core == 1))
        def _():
            pass_on(dyg, dy_send, dy_recv)

        @pl.when(k == 2 + core)
        def _():
            pass_on(xg, x_send, x_recv)

        @pl.when(k == 4)
        def _():
            pass_last(dyg, dy_send, dy_recv)

        @pl.when((k == 5) & (core == 0))
        def _():
            pass_last(xg, x_send, x_recv)

        @pl.when(k < 3)
        def _():
            fetch(k)

        @pl.loop(0, 3)
        def _(n):
            place = lax.broadcasted_iota(jnp.int32, (third, tok), 0) + n * third
            hit = place == pos_s[d]
            span = col(n * third, third)
            onehot[span, :] = jnp.where(hit, 1.0, 0.0).astype(BF16)
            grow[span, :] = jnp.sum(jnp.where(hit, gate_s[d], 0.0), axis=1, keepdims=True)

        move[...] = select(lax.broadcasted_iota(jnp.int32, (extra, extra), 0)
                           == lax.broadcasted_iota(jnp.int32, (extra, extra), 1) + shift_s[d][:, 0:1])
        @pl.when(k > 4)
        def _():
            for cp in keep(k - 2):
                cp.wait()

        local(xg.at[d], xst, 4).wait()
        local(dyg.at[d], dyst, 5).wait()

        @pl.loop(0, dim // TILE)
        def _(n):
            span = col(n * TILE, TILE)
            xr[mine, span] = mm(onehot[...], xst[:, span]).astype(BF16)
            dor[mine, span] = (grow[...] * mm(onehot[...], dyst[:, span])).astype(BF16)

        @pl.when((k == 2) | (k > 3))
        def _():
            send_back(k - 1)

        @pl.when((k == 3) | (k == 4))
        def _():
            fetch(k + 1)

        @pl.loop(0, ffn // TILE)
        def _(n):
            span = col(n * TILE, TILE)
            a = mm(xr[mine, :], wg[:, span])
            u = mm(xr[mine, :], wu[:, span])
            gh = mm(dor[mine, :], wd[span, :], NT)
            sig = jax.nn.sigmoid(a)
            act = a * sig
            hid[mine, span] = (act * u).astype(BF16)
            du[mine, span] = (gh * act).astype(BF16)
            da[mine, span] = (gh * u * sig * (1.0 + a * (1.0 - sig))).astype(BF16)

        @pl.when((k > 2) & (k < DEVS - 1))
        def _():
            for cp in keep(k):
                cp.start()

        merges(k, merge_load)

        @pl.loop(0, dim // TILE)
        def _(n):
            span = col(n * TILE, TILE)
            obuf[:, span] = mm(hid[mine, :], wd[:, span]).astype(BF16)

        local(obuf, out_stage.at[d], 0).start()
        ovv[0] = mm(move[...], obuf[base:, :]).astype(BF16)
        local(ovv.at[0], over_own.at[0, d], 2).start()

        merges(k, merge_add)

        @pl.loop(0, dim // TILE)
        def _(n):
            span = col(n * TILE, TILE)
            dbuf[:, span] = (mm(da[mine, :], wg[span, :], NT) + mm(du[mine, :], wu[span, :], NT)).astype(BF16)

        local(dbuf, dx_stage.at[d], 1).start()
        ovv[1] = mm(move[...], dbuf[base:, :]).astype(BF16)
        local(ovv.at[1], over_own.at[1, d], 3).start()
        merges(k, merge_send)

        @pl.when((k == 5) & (core == 1))
        def _():
            pass_last(xg, x_send, x_recv)

        @pl.when((k == 2) | (k == 5) | (k == 6))
        def _():
            fetch(k + 1)

        @pl.when(k == 0)
        def _():
            send_back(k)
            weight_grads(mine, lambda: None)

        @pl.when(k == 2)
        def _():
            weight_grads(slice(None), lambda: send_back(k))

    last = DEVS - 1
    send_back(last)
    for cp in keep(last - 1):
        cp.wait()
    for cp in bring(3):
        cp.start()

    @pl.when(core == 1)
    def _():
        merge_load(3)
        merge_add(3)

    def send_last():
        @pl.when(core == 1)
        def _():
            merge_send(3)

    weight_grads(region(last), send_last)
    for cp in bring(4):
        cp.start()
    for k in (3, 4):
        for cp in bring(k):
            cp.wait()
    weight_grads(slice(None), lambda: None)
    for k in (5, 6):
        for cp in bring(k):
            cp.start()
    for k in (5, 6):
        for cp in bring(k):
            cp.wait()
    weight_grads(slice(None), lambda: None)

    flag_copy = remote(flag_own, flag_peer, flag_sem.at[0], flag_sem.at[1], other, me)
    flag_copy.start()

    for acc, buf in ((accg, wg), (accu, wu), (accd, wd)):
        @pl.loop(0, acc.shape[0] // 128)
        def _(n, acc=acc, buf=buf):
            span = col(n * 128, 128)
            buf[span, :] = acc[span, :].astype(BF16)
    stores = [pltpu.make_async_copy(src, dst, load_sem.at[n])
              for n, (src, dst) in enumerate(((wg, gwg_ref), (wu, gwu_ref), (wd, gwd_ref)))]
    for cp in stores:
        cp.start()

    @pl.loop(0, tok // 128)
    def _(n):
        accg[col(n * 128, 128), :] = jnp.zeros((128, ffn), F32)
        accu[col(n * 128, 128), :] = jnp.zeros((128, ffn), F32)

    def back(k):
        return pl.ds(pl.multiple_of((k % 2) * base, 16), base)

    def load_back(k):
        d = nth_offset(k)

        @pl.when(k == 0)
        def _():
            local(out_stage.at[0, pl.ds(0, base)], obuf.at[back(k)], 0).start()

        @pl.when(k > 0)
        def _():
            out_copy(d).wait_recv()
            local(out_back.at[d], obuf.at[back(k)], k % 2).start()

        dx_copy(d).wait_recv()
        local(dx_back.at[d], dbuf.at[back(k)], 2 + k % 2).start()

    load_back(0)

    @pl.loop(0, DEVS)
    def _(k):
        d = nth_offset(k)
        local(out_back.at[d], obuf.at[back(k)], k % 2).wait()
        local(dx_back.at[d], dbuf.at[back(k)], 2 + k % 2).wait()

        @pl.when(k < DEVS - 1)
        def _():
            load_back(k + 1)

        @pl.loop(0, tok // 256)
        def _(n):
            over = col(n * 256, 256)
            place = lax.broadcasted_iota(jnp.int32, (256, base), 1)
            lane = lax.broadcasted_iota(jnp.int32, (256, DEVS), 1) == flip(me, d)

            def pick(ref):
                return jnp.sum(jnp.where(lane, ref[over, :], 0.0), axis=1, keepdims=True)

            accg[over, 0:dim] += pick(gate_y) * mm(select(place == pick(pos_y).astype(jnp.int32)), obuf[back(k), :])
            accu[over, 0:dim] += mm(select(place == pick(pos_x).astype(jnp.int32)), dbuf[back(k), :])

    held = [[xst.at[pl.ds(j * extra, extra)] if j < 3 else ovv.at[0] for j in range(4)],
            [dyst.at[pl.ds(j * extra, extra)] if j < 3 else ovv.at[1] for j in range(4)]]
    for j in range(4):
        for t in range(2):
            if t or j:
                sum_copy(t, j).wait_recv()
            local(over_back.at[t, j], held[t][j], 4 * t + j).start()
    for t in range(2):
        for j in range(4):
            local(over_back.at[t, j], held[t][j], 4 * t + j).wait()
        ovv[t] = sum(held[t][j][...].astype(F32) for j in range(4)).astype(BF16)

    @pl.loop(0, tok // 256)
    def _(n):
        over = col(n * 256, 256)
        place = lax.broadcasted_iota(jnp.int32, (256, extra), 1)
        at_y, at_x = over_y[over, :], over_x[over, :]

        def chosen(tab, c):
            return place == tab[:, c:c + 1].astype(jnp.int32)

        for c in range(2):
            accg[over, 0:dim] += at_y[:, 2 + c:3 + c] * mm(select(chosen(at_y, c)), ovv[0])
        accu[over, 0:dim] += mm(select(jnp.logical_or(chosen(at_x, 0), chosen(at_x, 1))), ovv[1])

    @pl.loop(0, tok // 128)
    def _(n):
        span = col(n * 128, 128)
        xst[span, :] = accg[span, 0:dim].astype(BF16)
        dyst[span, :] = accu[span, 0:dim].astype(BF16)

    flag_copy.wait()
    flag_own[...] = jnp.maximum(flag_own[...], flag_peer[...])
    ends = [local(xst, y_ref, 0), local(dyst, dx_ref, 1), local(flag_own, flag_ref, 2), local(pos_y, pos_y_ref, 3),
            local(gate_y, gate_y_ref, 4), local(pos_x, pos_x_ref, 5)]
    for cp in ends:
        cp.start()
    for cp in ends + stores:
        cp.wait()
    for sems, count in ((z_send, 2), (x_send, 14), (dy_send, 14)):
        for n in range(count):
            remote(xg.at[0, part[0]], xg.at[0, part[0]], sems.at[n], sems.at[n], st, me).wait_send()
    for d in range(DEVS):
        tab_copy(d).wait_send()
        dx_copy(d).wait_send()
        if d:
            out_copy(d).wait_send()
    for j in range(4):
        for t in range(2):
            pair_copy(t, 2 * j).wait_send()
            if t or j:
                sum_copy(t, j).wait_send()


def return_kernel(out_stage, dx_stage, pos_y, gate_y, pos_x, y_ref, dx_ref, out_back, dx_back,
                  acc_y, acc_x, obuf, dbuf, ybuf, xbuf, out_send, out_recv, dxs_send, dxs_recv, loc_sem):
    tok, dim = y_ref.shape
    rows = out_stage.shape[1]
    st, me = lax.axis_index('stage'), lax.axis_index('expert')
    greet(st, me)

    def out_copy(d):
        return pltpu.make_async_remote_copy(src_ref=out_stage.at[d], dst_ref=out_back.at[d], send_sem=out_send.at[d],
                                            recv_sem=out_recv.at[d], device_id=(st, flip(me, d)), device_id_type=MESH)

    def dx_copy(d):
        return pltpu.make_async_remote_copy(src_ref=dx_stage.at[d], dst_ref=dx_back.at[d], send_sem=dxs_send.at[d],
                                            recv_sem=dxs_recv.at[d], device_id=(1 - st, flip(me, d)), device_id_type=MESH)

    def local(src, dst, n):
        return pltpu.make_async_copy(src, dst, loc_sem.at[n])

    for d in range(DEVS):
        dx_copy(d).start()
        if d:
            out_copy(d).start()
    acc_y[...] = jnp.zeros_like(acc_y)
    acc_x[...] = jnp.zeros_like(acc_x)

    @pl.loop(0, DEVS)
    def _(d):
        @pl.when(d == 0)
        def _():
            local(out_stage.at[0], obuf, 0).start()

        @pl.when(d > 0)
        def _():
            out_copy(d).wait_recv()
            local(out_back.at[d], obuf, 0).start()

        dx_copy(d).wait_recv()
        local(dx_back.at[d], dbuf, 1).start()
        local(out_back.at[d], obuf, 0).wait()
        local(dx_back.at[d], dbuf, 1).wait()

        @pl.loop(0, tok // 256)
        def _(n):
            over = col(n * 256, 256)
            place = lax.broadcasted_iota(jnp.int32, (256, rows), 1)
            lane = lax.broadcasted_iota(jnp.int32, (256, DEVS), 1) == flip(me, d)

            def pick(ref):
                return jnp.sum(jnp.where(lane, ref[over, :], 0.0), axis=1, keepdims=True)

            acc_y[over, :] += pick(gate_y) * mm(select(place == pick(pos_y).astype(jnp.int32)), obuf[...])
            acc_x[over, :] += mm(select(place == pick(pos_x).astype(jnp.int32)), dbuf[...])

    ybuf[...] = acc_y[...].astype(BF16)
    xbuf[...] = acc_x[...].astype(BF16)
    ends = [local(ybuf, y_ref, 0), local(xbuf, dx_ref, 1)]
    for cp in ends:
        cp.start()
    for cp in ends:
        cp.wait()
    for d in range(DEVS):
        dx_copy(d).wait_send()
        if d:
            out_copy(d).wait_send()


def return_call(out_stage, dx_stage, pos_y, gate_y, pos_x):
    rows, dim = out_stage.shape[1:]
    tok = pos_y.shape[0]
    any_spec = pl.BlockSpec(memory_space=pl.ANY)
    vmem = pl.BlockSpec(memory_space=pltpu.VMEM)
    dma, vm, shape = pltpu.SemaphoreType.DMA, pltpu.VMEM, jax.ShapeDtypeStruct
    outs = pl.pallas_call(
        return_kernel,
        out_shape=[shape((tok, dim), BF16)] * 2 + [shape(out_stage.shape, BF16)] * 2,
        in_specs=[any_spec] * 2 + [vmem] * 3,
        out_specs=[any_spec] * 4,
        scratch_shapes=[vm((tok, dim), F32)] * 2 + [vm((rows, dim), BF16)] * 2 + [vm((tok, dim), BF16)] * 2
        + [dma((DEVS,))] * 4 + [dma((2,))],
        compiler_params=pltpu.CompilerParams(collective_id=1, has_side_effects=True),
    )(out_stage, dx_stage, pos_y, gate_y, pos_x)
    return outs[0], outs[1]


def moe_call(tab, x, dy, wg, wu, wd, cap, mean):
    tok, dim = x.shape
    ffn = wg.shape[1]
    rows = -(-cap // 48) * 48
    base = mean // 32 * 28
    extra = rows - base
    any_spec = pl.BlockSpec(memory_space=pl.ANY)
    vmem = pl.BlockSpec(memory_space=pltpu.VMEM)
    shape = jax.ShapeDtypeStruct
    out_shape = [shape((tok, dim), BF16)] * 2 + [shape(wg.shape, BF16), shape(wu.shape, BF16), shape(wd.shape, BF16)]
    out_shape += [shape((DEVS, rows, dim), BF16)] * 2 + [shape((tok, DEVS), F32)] * 3 + [shape((8, 128), F32)]
    out_shape += [shape((DEVS, tok, dim), BF16)] * 2 + [shape((DEVS, base, dim), BF16)] * 2
    out_shape += [shape((2, DEVS, extra, dim), BF16)] + [shape((2, 4, extra, dim), BF16)] * 3
    out_shape += [shape((4, rows, dim), BF16)] * 2 + [shape((4, rows, ffn), BF16)] * 3
    dma, vm = pltpu.SemaphoreType.DMA, pltpu.VMEM
    scratch = [
        vm((DEVS, 8, tok), F32), vm((DEVS, 1, tok), jnp.int32), vm((DEVS, 1, tok), F32), vm((DEVS, 1, 128), jnp.int32),
        vm((tok, DEVS), F32), vm((tok, DEVS), F32), vm((tok, DEVS), F32), vm((tok, DEVS), F32), vm((tok, DEVS), F32),
        vm((8, 128), F32), vm((8, 128), F32),
        vm((dim, ffn), BF16), vm((dim, ffn), BF16), vm((ffn, dim), BF16),
        vm((dim, ffn), F32), vm((dim, ffn), F32), vm((ffn, dim), F32),
        vm((tok, dim), BF16), vm((tok, dim), BF16), vm((rows, tok), BF16), vm((rows, 1), F32),
        vm((2 * rows, dim), BF16), vm((2 * rows, dim), BF16), vm((2 * rows, ffn), BF16), vm((2 * rows, ffn), BF16), vm((2 * rows, ffn), BF16),
        vm((rows, dim), BF16), vm((rows, dim), BF16), vm((2, extra, dim), BF16), vm((2, extra, dim), BF16), vm((2, extra, dim), BF16), vm((extra, extra), BF16),
        dma((3,)), dma((DEVS,)), dma((DEVS,)), dma((2,)), dma((14,)), dma((14,)), dma((DEVS, 2)), dma((DEVS, 2)),
        dma((DEVS,)), dma((DEVS,)), dma((DEVS,)), dma((DEVS,)), dma((2, 4)), dma((2, 4)), dma((2, 4)), dma((2, 4)), dma((2,)), dma((10,)), dma((10,)),
    ]
    return pl.pallas_call(
        functools.partial(moe_kernel, rows, base),
        out_shape=out_shape,
        in_specs=[vmem] + [any_spec] * 5,
        out_specs=[any_spec] * len(out_shape),
        scratch_shapes=scratch,
        compiler_params=pltpu.CompilerParams(collective_id=0, has_side_effects=True, vmem_limit_bytes=67043328),
    )(tab, x, dy, wg, wu, wd)


def solution(mesh):
    stages, ep_size = mesh.shape['stage'], mesh.shape['expert']
    assert stages == 2 and ep_size == DEVS
    tok_spec = P('stage', 'expert', None)
    w_spec = P('stage', 'expert', None, None)

    def device_fn(x_acts, expert_ids, gate_vals, w_gate, w_up, w_down, grad_out):
        tok, top_k = expert_ids.shape[1:]
        cap = 2 * tok * top_k // (w_gate.shape[1] * ep_size) + 1
        tab = jnp.concatenate([expert_ids[0].T.astype(F32), gate_vals[0].T, jnp.zeros((4, tok), F32)], axis=0)
        outs = moe_call(tab, x_acts[0], grad_out[0], w_gate[0, 0], w_up[0, 0], w_down[0, 0], cap, tok * top_k // ep_size)
        y, dx, gwg, gwu, gwd = outs[:5]
        y, dx = lax.cond(outs[10][0, 0] > 0, return_call, lambda *_: (y, dx), *outs[5:10])
        return y[None], dx[None], gwg[None, None], gwu[None, None], gwd[None, None]

    return jax.shard_map(device_fn, mesh=mesh, in_specs=(tok_spec, tok_spec, tok_spec, w_spec, w_spec, w_spec, tok_spec), out_specs=(tok_spec, tok_spec, w_spec, w_spec, w_spec), check_vma=False)
```
